128 devices in a mesh: rep: 1, dp: 128 (over x, y, z, core).
Axes of the slice: x: 4, y: 4, z: 4, core: 2. Of those that a mesh axis runs over, the one named last changes fastest.
Arguments:
- g_w_gate: bfloat16 [128, 2, 640, 3200], P(('rep', 'dp'))
- g_w_up: bfloat16 [128, 2, 640, 3200], P(('rep', 'dp'))
- g_w_down: bfloat16 [128, 2, 3200, 640], P(('rep', 'dp'))
- w_gate: bfloat16 [2, 640, 3200], replicated
- w_up: bfloat16 [2, 640, 3200], replicated
- w_down: bfloat16 [2, 3200, 640], replicated
- m_w_gate: float32 [2, 640, 3200], P(None, 'dp')
- m_w_up: float32 [2, 640, 3200], P(None, 'dp')
- m_w_down: float32 [2, 3200, 640], P(None, 'dp')
- v_w_gate: float32 [2, 640, 3200], P(None, 'dp')
- v_w_up: float32 [2, 640, 3200], P(None, 'dp')
- v_w_down: float32 [2, 3200, 640], P(None, 'dp')
Outputs:
- output 1: bfloat16 [2, 640, 3200], P('rep')
- output 2: bfloat16 [2, 640, 3200], P('rep')
- output 3: bfloat16 [2, 3200, 640], P('rep')
- output 4: float32 [2, 640, 3200], P('rep', 'dp')
- output 5: float32 [2, 640, 3200], P('rep', 'dp')
- output 6: float32 [2, 3200, 640], P('rep', 'dp')
- output 7: float32 [2, 640, 3200], P('rep', 'dp')
- output 8: float32 [2, 640, 3200], P('rep', 'dp')
- output 9: float32 [2, 3200, 640], P('rep', 'dp')
All inputs are finite; a program needn't handle non-finite values.
Results may differ from the reference program's by a relative error of at most 0.022.
Values are sent between devices in bfloat16 or wider.
A program may use at most 1.5 GiB of HBM per device.

```python
import jax
import jax.numpy as jnp
from jax import lax

DEVICES = 128
D = 640
FF = 3200
LAYERS = 2
NAMES = ("w_gate", "w_up", "w_down")
SHAPES = {"w_gate": (LAYERS, D, FF), "w_up": (LAYERS, D, FF), "w_down": (LAYERS, FF, D)}


def setup_inputs(seed: int = 0, part: int = 0) -> dict:
    kz, *keys = jax.random.split(jax.random.key(seed), 1 + 5 * len(NAMES))
    loud = 2.0 ** jax.random.uniform(kz, (), jnp.float32, -1.0, 1.0)
    drawn = {}
    for name, key, both in zip(NAMES, keys[:3], keys[3:6], strict=True):
        own = jax.random.normal(jax.random.fold_in(key, part), (DEVICES, *SHAPES[name]), jnp.float32)
        shared = jax.random.normal(jax.random.fold_in(both, part), SHAPES[name], jnp.float32)
        drawn["g_" + name] = (loud * (0.7 * shared / DEVICES + 0.7 * own * DEVICES**-0.5)).astype(jnp.bfloat16)
    for name, key in zip(NAMES, keys[6:9], strict=True):
        drawn[name] = (jax.random.normal(key, SHAPES[name], jnp.float32) * SHAPES[name][1] ** -0.5).astype(jnp.bfloat16)
    for name, key in zip(NAMES, keys[9:12], strict=True):
        drawn["m_" + name] = loud * 0.5 * jax.random.normal(key, SHAPES[name], jnp.float32)
    for name, key in zip(NAMES, keys[12:15], strict=True):
        drawn["v_" + name] = loud * loud * jax.random.uniform(key, SHAPES[name], jnp.float32, 0.5, 1.5)
    return drawn


def adamw(w, m, v, g):
    m = 0.9 * m + 0.1 * g
    v = 0.95 * v + 0.05 * g * g
    step = m * lax.rsqrt(v + 1e-8) + 0.1 * w
    return (w - 0.02 * step).astype(jnp.bfloat16), m, v


def reference(g_w_gate, g_w_up, g_w_down, w_gate, w_up, w_down, m_w_gate, m_w_up, m_w_down, v_w_gate, v_w_up, v_w_down):
    def total(terms):
        return lax.scan(lambda so_far, term: (so_far + term.astype(jnp.float32), None), jnp.zeros(terms.shape[1:], jnp.float32), terms)[0]

    gradients = [total(terms).astype(jnp.bfloat16).astype(jnp.float32) for terms in (g_w_gate, g_w_up, g_w_down)]
    new = [
        adamw(w.astype(jnp.float32), m, v, g)
        for w, m, v, g in zip((w_gate, w_up, w_down), (m_w_gate, m_w_up, m_w_down), (v_w_gate, v_w_up, v_w_down), gradients, strict=True)
    ]
    return tuple(one[which] for which in range(3) for one in new)
```

```python
import jax
import jax.numpy as jnp
from jax import lax
from jax.experimental import pallas as pl
from jax.experimental.pallas import tpu as pltpu
from jax.sharding import PartitionSpec as P

BF, F32 = jnp.bfloat16, jnp.float32
WA = 3328
WC = 768
OFF = (2, 3, 1, 0)
HBM = pltpu.MemorySpace.HBM
VMEM = pltpu.MemorySpace.VMEM


def adamw(w, m, v, g):
    m = 0.9 * m + 0.1 * g
    v = 0.95 * v + 0.05 * g * g
    step = m * lax.rsqrt(v + 1e-8) + 0.1 * w
    return (w - 0.02 * step).astype(jnp.bfloat16), m, v


class Place:
    def __init__(self):
        me = lax.axis_index("dp")
        self.c = lax.rem(me, 2)
        self.z = lax.rem(me // 2, 4)
        self.y = lax.rem(me // 8, 4)
        self.x = me // 32
        self.g = lax.rem(me, 8)
        self.partner = self.dev(c=1 - self.c)

    def dev(self, x=None, y=None, z=None, c=None):
        x = self.x if x is None else x
        y = self.y if y is None else y
        z = self.z if z is None else z
        c = self.c if c is None else c
        return {"dp": ((x * 4 + y) * 4 + z) * 2 + c}

    def step(self, dim, by):
        return self.dev(**{dim: lax.rem(getattr(self, dim) + by, 4)})

    def group(self):
        out = [(self.z, 1 - self.c)]
        for dz in (1, 2, 3):
            zz = lax.rem(self.z + dz, 4)
            out += [(zz, self.c), (zz, 1 - self.c)]
        return out

    def barrier(self):
        sem = pltpu.get_barrier_semaphore()
        peers = [self.dev(z=z, c=c) for z, c in self.group()]
        peers += [self.step(d, by) for d in ("x", "y") for by in (1, 3)]
        for peer in peers:
            pl.semaphore_signal(sem, inc=1, device_id=peer, device_id_type=pl.DeviceIdType.MESH)
        pl.semaphore_wait(sem, len(peers))


class Sender:
    def __init__(self, send, recv):
        self.send, self.recv, self.n, self.all = send, recv, 0, []

    def start(self, src, dst, device):
        copy = pltpu.make_async_remote_copy(
            src_ref=src,
            dst_ref=dst,
            send_sem=self.send.at[self.n],
            recv_sem=self.recv.at[self.n],
            device_id=device,
            device_id_type=pl.DeviceIdType.MESH,
        )
        copy.start()
        self.n += 1
        self.all.append(copy)
        return copy

    def drain(self):
        for copy in self.all:
            copy.wait_send()


def rows(start, n):
    return pl.ds(pl.multiple_of(start, 8), n)


def total(refs, sl):
    acc = refs[0][sl].astype(F32)
    for r in refs[1:]:
        acc = acc + r[sl].astype(F32)
    return acc


def vadd(dst, refs, n, step):
    def body(i, carry):
        sl = (rows(i * step, step), slice(None))
        dst[sl] = total(refs, sl).astype(dst.dtype)
        return carry

    lax.fori_loop(0, n // step, body, 0)


def interleave(*programs):
    live = list(programs)
    while live:
        for p in list(live):
            try:
                next(p)
            except StopIteration:
                live.remove(p)


def reduce_kernel(g_gate, g_up, g_down, o_gate, o_up, o_down, own_a, par_a, own_b, par_b, own_c, par_c, r1a, r2a, r1b, r2b, r1c, r2c,
                  s1a, s2a, s1b, s2b, s1c, s2c, t1c, t2c, f_a, f_b, f_c, snd_a, snd_b, snd_c, rcv_a, rcv_b, rcv_c, send, recv, local):
    at = Place()
    x, y, z, c = at.x, at.y, at.z, at.c
    net = Sender(send, recv)
    loads = [0]

    rel = lambda base, j: lax.rem(base + OFF[j], 4)

    def item_a(ref, k, j):
        return ref.at[rows(160 * k + 40 * rel(y, j), 40), :]

    def item_b(ref, k, j):
        return ref.at[rows(200 * k + 800 * rel(x, j), 200), :]

    def item_c(ref, k, j):
        return ref.at[k, rows(160 * rel(x, j), 160), :]

    def src_a(layer, k, j):
        return g_up.at[0, layer, rows(160 * k + 40 * rel(y, j), 40), :]

    def src_b(layer, k, j):
        return g_down.at[0, layer, rows(200 * k + 800 * rel(x, j), 200), :]

    def src_c(layer, k, j):
        return g_gate.at[0, layer, rows(160 * rel(x, j), 160), pl.ds(pl.multiple_of(WC * k, 128), WC)]

    def dst_a(ref, k, j):
        return ref.at[rows(160 * k + 40 * rel(y, j), 40), pl.ds(0, 3200)]

    colours = {
        "a": (own_a, par_a, item_a, src_a, dst_a, x, "x", r1a, r2a, 40, 8),
        "b": (own_b, par_b, item_b, src_b, item_b, y, "y", r1b, r2b, 200, 40),
        "c": (own_c, par_c, item_c, src_c, item_c, z, "z", r1c, r2c, 160, 32),
    }

    def load(src, dst):
        copy = pltpu.make_async_copy(src, dst, local.at[loads[0]])
        copy.start()
        loads[0] += 1
        return copy

    near = {}
    tail = (0, c, slice(None), pl.ds(3072, 128))
    near["tail"] = load(g_gate.at[tail], own_a.at[:, pl.ds(3200, 128)])
    order = [(2, j) for j in (0, 2, 1, 3)] + [(1, 2), (3, 0), (1, 3), (3, 1), (1, 0), (3, 2), (1, 1), (3, 3)] + [(0, j) for j in (0, 2, 1, 3)]
    for dk, j in order:
        for n, (own, par, item, src, dst, k0, *_) in colours.items():
            k = lax.rem(k0 + dk, 4)
            near[n, dk, j] = load(src(c, k, j), dst(own, k, j))
    at.barrier()
    far = {}
    tail = (0, 1 - c, slice(None), pl.ds(3072, 128))
    far["tail"] = net.start(g_gate.at[tail], par_a.at[:, pl.ds(3200, 128)], at.partner)
    for dk, j in order:
        for n, (own, par, item, src, dst, k0, *_) in colours.items():
            k = lax.rem(k0 + dk, 4)
            far[n, dk, j] = net.start(src(1 - c, k, j), dst(par, k, j), at.partner)
    near["tail"].wait()
    far["tail"].wait_recv()

    def first(n):
        own, par, item, src, dst, k0, dim, r1, r2, height, step = colours[n]
        up, down = at.step(dim, 1), at.step(dim, 3)
        k2, kp, km = (lax.rem(k0 + d, 4) for d in (2, 1, 3))
        one, two = {}, {}
        for j in (0, 2, 1, 3):
            yield
            near[n, 2, j].wait()
            far[n, 2, j].wait_recv()
            here = item(own, k2, j)
            vadd(here, (here, item(par, k2, j)), height, step)
            one[j] = net.start(here, r1.at[j], up if j < 2 else down)
        for dk, j in ((1, 2), (3, 0), (1, 3), (3, 1)):
            yield
            near[n, dk, j].wait()
            far[n, dk, j].wait_recv()
            k = kp if dk == 1 else km
            here = item(own, k, j)
            vadd(here, (here, item(par, k, j)), height, step)
            two[dk, j] = net.start(here, r2.at[j if dk == 1 else 4 + j], up if dk == 1 else down)
        for dk, j in ((1, 0), (3, 2), (1, 1), (3, 3)):
            yield
            near[n, dk, j].wait()
            far[n, dk, j].wait_recv()
            one[j].wait_recv()
            k = kp if dk == 1 else km
            here = item(own, k, j)
            vadd(here, (here, item(par, k, j), r1.at[j]), height, step)
            two[dk, j] = net.start(here, r2.at[j if dk == 1 else 4 + j], up if dk == 1 else down)
        for j in (0, 2, 1, 3):
            yield
            near[n, 0, j].wait()
            far[n, 0, j].wait_recv()
            two[1, j].wait_recv()
            two[3, j].wait_recv()
            here = item(own, k0, j)
            vadd(here, (here, item(par, k0, j), r2.at[j], r2.at[4 + j]), height, step)
            yield j

    def later(n, dim, block, halves, r1, r2, ready, step, done):
        up, down = at.step(dim, 1), at.step(dim, 3)
        two = {}
        for j in ready:
            yield
            if j == 0:
                a = net.start(halves(block(0), 0), halves(r1.at[0], 0, True), up)
                b = net.start(halves(block(0), 1), halves(r1.at[1], 1, True), down)
            if j == 2:
                two[0] = net.start(halves(block(2), 1), halves(r2.at[0], 1), up)
            if j == 1:
                two[1] = net.start(halves(block(1), 0), halves(r2.at[1], 0), down)
        yield
        a.wait_recv()
        here = halves(block(2), 0)
        vadd(here, (here, halves(r1.at[0], 0, True)), here.shape[0], 8)
        two[2] = net.start(here, halves(r2.at[0], 0), up)
        yield
        b.wait_recv()
        here = halves(block(1), 1)
        vadd(here, (here, halves(r1.at[1], 1, True)), here.shape[0], 8)
        two[3] = net.start(here, halves(r2.at[1], 1), down)
        yield
        for i in range(4):
            two[i].wait_recv()
        vadd(done, (block(3), r2.at[0], r2.at[1]), block(3).shape[0], step)
        yield

    def steps(gen):
        for j in gen:
            yield j

    def halves_cols(w):
        def cut(ref, h, packed=False):
            return ref if packed else ref.at[:, pl.ds(h * w, w)]

        return cut

    def halves_rows(n0, n1):
        def cut(ref, h, packed=False):
            return ref.at[pl.ds(0, (n0, n1)[h]), :] if packed else ref.at[pl.ds((0, n0)[h], (n0, n1)[h]), :]

        return cut

    def spread(n, full, blocks, height, snd, rcv):
        sent = []
        for k in range(8):
            snd[k] = full[pl.ds(blocks * k, height), :].astype(BF)
        for zz, cc in at.group():
            s = 2 * zz + cc
            sent.append(net.start(snd.at[s], rcv.at[at.g], at.dev(z=zz, c=cc)))
        rcv[at.g] = snd[at.g]
        return sent

    sent = {}

    def colour_a():
        f_a[pl.ds(40, 8), :] = jnp.zeros((8, WA), F32)
        yield from later("a", "y", lambda j: item_a(own_a, x, j), halves_cols(WA // 2), s1a, s2a, first("a"), 8, f_a)
        sent["a"] = spread("a", f_a, 5, 8, snd_a, rcv_a)

    def colour_b():
        f_b[pl.ds(200, 8), :] = jnp.zeros((8, 640), F32)
        yield from later("b", "x", lambda j: item_b(own_b, y, j), halves_rows(104, 96), s1b, s2b, first("b"), 40, f_b)
        sent["b"] = spread("b", f_b, 25, 32, snd_b, rcv_b)

    def colour_c():
        f_c[pl.ds(40, 8), :] = jnp.zeros((8, WC), F32)
        yield from later("c", "x", lambda j: item_c(own_c, z, j), halves_rows(80, 80), s1c, s2c, first("c"), 32, item_c(own_c, z, 3))
        block = lambda j: own_c.at[z, rows(160 * x + 40 * rel(y, j), 40), :]
        yield from later("c", "y", block, halves_cols(WC // 2), t1c, t2c, iter((0, 2, 1, 3)), 8, f_c)
        sent["c"] = spread("c", f_c, 5, 8, snd_c, rcv_c)

    interleave(colour_a(), colour_b(), colour_c())

    for n in ("a", "b", "c"):
        for copy in sent[n]:
            copy.wait_recv()
    for layer in range(2):
        acc = rcv_a[layer].astype(F32)
        low = rcv_b[layer].astype(F32)
        for zz in range(1, 4):
            acc = acc + rcv_a[2 * zz + layer].astype(F32)
            low = low + rcv_b[2 * zz + layer].astype(F32)
        o_up[layer] = acc[:, :3200].astype(BF)
        o_gate[layer, :, pl.ds(3072, 128)] = acc[:, 3200:].astype(BF)
        o_down[layer] = low.astype(BF)
        for zz in range(4):
            o_gate[layer, :, pl.ds(WC * zz, WC)] = rcv_c[2 * zz + layer]
    net.drain()


def gather_kernel(w_a, w_b, w_c, o_a, o_b, o_c, g_a, g_b, g_c, f_a, f_b, f_c, send, recv):
    at = Place()
    x, y, z, c = at.x, at.y, at.z, at.c
    net = Sender(send, recv)
    at.barrier()
    rel = lambda base, j: lax.rem(base + OFF[j], 4)
    cross = []

    def window(zz):
        return pl.ds(pl.multiple_of(WC * zz, 128), WC)

    sent = {"a": [], "b": [], "c": []}
    for zz, cc in at.group():
        device = at.dev(z=zz, c=cc)
        sent["c"].append(net.start(w_c.at[cc, :, window(zz)], g_c.at[at.g], device))
        sent["a"].append(net.start(w_a.at[cc], g_a.at[at.g], device))
        sent["b"].append(net.start(w_b.at[cc], g_b.at[at.g], device))
    g_c[at.g] = w_c[c, :, window(z)]
    g_a[at.g] = w_a[c]
    g_b[at.g] = w_b[c]

    def over(ref):
        cross.append(net.start(ref, ref, at.partner))

    def build(n, blocks, got, full, out):
        for copy in sent[n]:
            copy.wait_recv()
        for k in range(8):
            full[pl.ds(blocks * k, blocks), :] = got[k].astype(F32)[:blocks]
        out[...] = full[...].astype(BF)

    def small(dim, block, halves):
        up, down = at.step(dim, 1), at.step(dim, 3)
        mine = block(3)
        m0 = net.start(halves(mine, 0), halves(mine, 0), up)
        p1 = net.start(halves(mine, 1), halves(mine, 1), down)
        m1 = net.start(halves(mine, 1), halves(mine, 1), up)
        p0 = net.start(halves(mine, 0), halves(mine, 0), down)
        yield 3
        m0.wait_recv()
        here = halves(block(1), 0)
        f0 = net.start(here, here, up)
        p1.wait_recv()
        here = halves(block(2), 1)
        f1 = net.start(here, here, down)
        yield
        m1.wait_recv()
        yield 1
        p0.wait_recv()
        yield 2
        f0.wait_recv()
        f1.wait_recv()
        yield 0

    def large(dim, k0, item, ready):
        up, down = at.step(dim, 1), at.step(dim, 3)
        kp, km, k2 = (lax.rem(k0 + d, 4) for d in (1, 3, 2))
        fm, fp, order = {}, {}, []
        for j in ready:
            if j is not None:
                here = item(k0, j)
                fm[j] = net.start(here, here, up)
                fp[j] = net.start(here, here, down)
                over(here)
                order.append(j)
            yield
        f2 = {}
        for j in order:
            fm[j].wait_recv()
            here = item(km, j)
            if j < 2:
                f2[j] = net.start(here, here, up)
            over(here)
            yield
            fp[j].wait_recv()
            here = item(kp, j)
            if j >= 2:
                f2[j] = net.start(here, here, down)
            over(here)
            yield
        for j in order:
            f2[j].wait_recv()
            over(item(k2, j))
            yield

    def cols(w):
        return lambda ref, h: ref.at[:, pl.ds(h * w, w)]

    def parts(n0, n1):
        return lambda ref, h: ref.at[pl.ds((0, n0)[h], (n0, n1)[h]), :]

    item_a = lambda k, j: o_a.at[c, rows(160 * k + 40 * rel(y, j), 40), :]
    item_b = lambda k, j: o_b.at[c, rows(200 * k + 800 * rel(x, j), 200), :]
    item_c = lambda k, j: o_c.at[c, k, rows(160 * rel(x, j), 160), :]

    def colour_a():
        build("a", 5, g_a, f_a, item_a(x, 3))
        yield from large("x", x, item_a, small("y", lambda j: item_a(x, j), cols(WA // 2)))

    def colour_b():
        build("b", 25, g_b, f_b, item_b(y, 3))
        yield from large("y", y, item_b, small("x", lambda j: item_b(y, j), parts(104, 96)))

    def colour_c():
        block = lambda j: o_c.at[c, z, rows(160 * x + 40 * rel(y, j), 40), :]
        build("c", 5, g_c, f_c, block(3))
        for _ in small("y", block, cols(WC // 2)):
            yield
        yield from large("z", z, item_c, small("x", lambda j: item_c(z, j), parts(80, 80)))

    interleave(colour_c(), colour_a(), colour_b())
    for copy in cross:
        copy.wait_recv()
    net.drain()


def write_kernel(a, b, c, gate, up, down, sem):
    copies = [(b.at[l], down.at[l]) for l in range(2)]
    copies += [(a.at[l, :, pl.ds(0, 3200)], up.at[l]) for l in range(2)]
    copies += [(c.at[l, k], gate.at[l, :, pl.ds(WC * k, WC)]) for l in range(2) for k in range(4)]
    copies += [(a.at[l, :, pl.ds(3200, 128)], gate.at[l, :, pl.ds(3072, 128)]) for l in range(2)]
    copies = [pltpu.make_async_copy(s, d, sem.at[i]) for i, (s, d) in enumerate(copies)]
    for copy in copies:
        copy.start()
    for copy in copies:
        copy.wait()


def spec(space, n):
    return [pl.BlockSpec(memory_space=space)] * n


def solution(mesh):
    def step(*arrays):
        terms, weights, m, v = (arrays[i : i + 3] for i in (0, 3, 6, 9))
        sums = pl.pallas_call(
            reduce_kernel,
            out_shape=[VMEM((2, 8, 3200), BF), VMEM((2, 8, 3200), BF), VMEM((2, 32, 640), BF)],
            in_specs=spec(HBM, 3),
            out_specs=spec(VMEM, 3),
            scratch_shapes=[
                *[VMEM((640, WA), BF)] * 2,
                *[VMEM((3200, 640), BF)] * 2,
                *[VMEM((4, 640, WC), BF)] * 2,
                *[VMEM((n, *s), BF) for s in ((40, WA), (200, 640), (160, WC)) for n in (4, 8)],
                VMEM((2, 40, WA // 2), BF),
                VMEM((2, 40, WA), BF),
                VMEM((2, 104, 640), BF),
                VMEM((2, 200, 640), BF),
                VMEM((2, 80, WC), BF),
                VMEM((2, 160, WC), BF),
                VMEM((2, 40, WC // 2), BF),
                VMEM((2, 40, WC), BF),
                VMEM((48, WA), F32),
                VMEM((208, 640), F32),
                VMEM((48, WC), F32),
                *[VMEM((8, *s), BF) for s in ((8, WA), (32, 640), (8, WC))] * 2,
                pltpu.SemaphoreType.DMA((140,)),
                pltpu.SemaphoreType.DMA((140,)),
                pltpu.SemaphoreType.DMA((49,)),
            ],
            compiler_params=pltpu.CompilerParams(collective_id=0, has_side_effects=True, vmem_limit_bytes=56 * 2**20),
            name="reduce",
        )(*terms)
        gradients = [s[:, : one.shape[1]].astype(F32) for s, one in zip(sums, m, strict=True)]
        me = lax.axis_index("dp")
        own = [lax.dynamic_slice_in_dim(w, me * one.shape[1], one.shape[1], 1).astype(F32) for w, one in zip(weights, m, strict=True)]
        new = [adamw(w, m, v, g) for w, m, v, g in zip(own, m, v, gradients, strict=True)]
        gate, up, down = (one[0] for one in new)
        w_a = jnp.pad(jnp.concatenate([up, gate[:, :, 3072:]], 2), ((0, 0), (0, 3), (0, 0)))
        w_b = jnp.pad(down, ((0, 0), (0, 7), (0, 0)))
        w_c = jnp.pad(gate[:, :, :3072], ((0, 0), (0, 3), (0, 0)))
        whole = pl.pallas_call(
            gather_kernel,
            out_shape=[VMEM((2, 640, WA), BF), VMEM((2, 3200, 640), BF), VMEM((2, 4, 640, WC), BF)],
            in_specs=spec(VMEM, 3),
            out_specs=spec(VMEM, 3),
            scratch_shapes=[
                VMEM((8, 8, WA), BF),
                VMEM((8, 32, 640), BF),
                VMEM((8, 8, WC), BF),
                VMEM((40, WA), F32),
                VMEM((200, 640), F32),
                VMEM((40, WC), F32),
                pltpu.SemaphoreType.DMA((140,)),
                pltpu.SemaphoreType.DMA((140,)),
            ],
            compiler_params=pltpu.CompilerParams(collective_id=1, has_side_effects=True, vmem_limit_bytes=8 * 2**20),
            name="gather",
        )(w_a, w_b, w_c)
        whole = pl.pallas_call(
            write_kernel,
            out_shape=[jax.ShapeDtypeStruct(w.shape, BF) for w in weights],
            in_specs=spec(VMEM, 3),
            out_specs=spec(HBM, 3),
            scratch_shapes=[pltpu.SemaphoreType.DMA((14,))],
            compiler_params=pltpu.CompilerParams(vmem_limit_bytes=2**20),
            name="write",
        )(*whole)
        return (*whole, *(one[1] for one in new), *(one[2] for one in new))

    all_of, cut = P(None, None, None), P(None, "dp", None)
    return jax.shard_map(
        step,
        mesh=mesh,
        in_specs=(P(("rep", "dp"), None, None, None),) * 3 + (all_of,) * 3 + (cut,) * 6,
        out_specs=(P("rep", None, None),) * 3 + (P("rep", "dp", None),) * 6,
        check_vma=False,
    )
```

```python
import jax
import jax.numpy as jnp
from jax import lax
from jax.experimental import pallas as pl
from jax.experimental.pallas import tpu as pltpu
from jax.sharding import PartitionSpec as P

ALL = slice(None)
BF, F32 = jnp.bfloat16, jnp.float32
D, FF, LANES, GROUP, OTHERS = 640, 3200, 128, 8, 7
OWN_A, OWN_B = 5, 25
BLOCK, SLAB, TALL, TALL4 = 40, 160, 200, 800
BLOCK_PAD, TALL_PAD = 48, 208
WIN, EDGE = 768, 3072
SHARE = 1
UC = 128 * SHARE
UA = 3200 - 4 * UC
WA = UA + 128
WC = 768 + UC
PLAN = "cab" * 10 + "pppppppppppppp" + "cab" * 6
PLAN += "cabcab" + "abc" + "a" + "ccc" + "b" + "aA" + "c" + "b" + "cc" + "B" + "c" + "Cab" + "ab" + "c" + "ABC" + "abc" + "ABC" + "abc" + "ABC"
PLAN += "f" * 7
SEND, RECV, LOCAL = 26, 142, 34
OFF = (2, 3, 1, 0)
HBM = pltpu.MemorySpace.HBM
VMEM = pltpu.MemorySpace.VMEM


def adamw(w, m, v, g):
    m = 0.9 * m + 0.1 * g
    v = 0.95 * v + 0.05 * g * g
    step = m * lax.rsqrt(v + 1e-8) + 0.1 * w
    return (w - 0.02 * step).astype(jnp.bfloat16), m, v


class Place:
    def __init__(self):
        me = lax.axis_index("dp")
        self.c = lax.rem(me, 2)
        self.z = lax.rem(me // 2, 4)
        self.y = lax.rem(me // GROUP, 4)
        self.x = me // 32
        self.g = lax.rem(me, GROUP)
        self.partner = self.dev(c=1 - self.c)

    def dev(self, x=None, y=None, z=None, c=None):
        x = self.x if x is None else x
        y = self.y if y is None else y
        z = self.z if z is None else z
        c = self.c if c is None else c
        return {"dp": ((x * 4 + y) * 4 + z) * 2 + c}

    def step(self, dim, by):
        return self.dev(**{dim: lax.rem(getattr(self, dim) + by, 4)})

    def group(self):
        out = [(self.z, 1 - self.c)]
        for dz in (1, 2, 3):
            zz = lax.rem(self.z + dz, 4)
            out += [(zz, self.c), (zz, 1 - self.c)]
        return out

    def barrier(self):
        sem = pltpu.get_barrier_semaphore()
        peers = [self.dev(z=z, c=c) for z, c in self.group()]
        peers += [self.step(d, by) for d in ("x", "y") for by in (1, 3)]
        for peer in peers:
            pl.semaphore_signal(sem, inc=1, device_id=peer, device_id_type=pl.DeviceIdType.MESH)
        pl.semaphore_wait(sem, len(peers))


class Sender:
    def __init__(self, send, recv):
        self.send, self.recv, self.n, self.groups, self.shared = send, recv, 0, {}, {}

    def start(self, src, dst, device, group, together=None):
        mine = self.groups.setdefault(group, len(self.groups))
        if together is None or together not in self.shared:
            got = self.n
            self.n += 1
            if together is not None:
                self.shared[together] = got
        else:
            got = self.shared[together]
        copy = pltpu.make_async_remote_copy(
            src_ref=src,
            dst_ref=dst,
            send_sem=self.send.at[mine],
            recv_sem=self.recv.at[got],
            device_id=device,
            device_id_type=pl.DeviceIdType.MESH,
        )
        copy.start()
        return copy

    def arrived(self, together, like):
        pltpu.make_async_copy(like, like, self.recv.at[self.shared[together]]).wait()

    def drain(self, sizes):
        for group, n in self.groups.items():
            like = sizes[group]
            pltpu.make_async_copy(like, like, self.send.at[n]).wait()


def rows(start, n):
    return pl.ds(pl.multiple_of(start, GROUP), n)


def total(refs, sl):
    acc = refs[0][sl].astype(F32)
    for r in refs[1:]:
        acc = acc + r[sl].astype(F32)
    return acc


def vadd(dst, refs, n, step):
    def body(i, carry):
        sl = (rows(i * step, step), ALL)
        dst[sl] = total(refs, sl).astype(dst.dtype)
        return carry

    lax.fori_loop(0, n // step, body, 0)


def interleave(plan, release, **programs):
    live = dict(programs)

    def advance(n):
        try:
            next(live[n])
        except StopIteration:
            del live[n]

    for n in plan:
        if n in release:
            release[n]()
        elif n in live:
            advance(n)
    while live:
        for n in list(live):
            advance(n)


def step_kernel(g_gate, g_up, g_down, w_gate, w_up, w_down, m_gate, m_up, m_down, v_gate, v_up, v_down,
                o_a, o_b, o_c, om_gate, om_up, om_down, ov_gate, ov_up, ov_down,
                own_a, own_b, own_c, ra, rb, rc, s1a, s2a, s1b, s2b, s1c, s2c, t1c, t2c, f_a, f_b, f_c,
                snd_a, snd_b, snd_c, rcv_a, rcv_b, rcv_c, new_a, new_b, new_c, got_a, got_b, got_c,
                wb_gate, wb_up, wb_down, fw_wide, fw_tall, w2_gate, w2_up, w2_down, m2_gate, m2_up, m2_down, v2_gate, v2_up, v2_down,
                send, recv, local):
    at = Place()
    x, y, z, c = at.x, at.y, at.z, at.c
    net = Sender(send, recv)
    loads = [0]
    rel = lambda base, j: lax.rem(base + OFF[j], 4)
    cols = lambda start, n: pl.ds(pl.multiple_of(start, LANES), n)

    def item_a(ref, k, j):
        return ref.at[rows(SLAB * k + BLOCK * rel(y, j), BLOCK), :]

    def item_b(ref, k, j):
        return ref.at[rows(TALL * k + TALL4 * rel(x, j), TALL), :]

    def item_c(ref, k, j):
        return ref.at[k, rows(SLAB * rel(x, j), SLAB), :]

    def moves_a(layer, ref, k, j):
        sl = rows(SLAB * k + BLOCK * rel(y, j), BLOCK)
        return [(g_up.at[0, layer, sl, pl.ds(0, UA)], ref.at[sl, pl.ds(0, UA)])]

    def moves_b(layer, ref, k, j):
        return [(g_down.at[0, layer, rows(TALL * k + TALL4 * rel(x, j), TALL), :], item_b(ref, k, j))]

    def moves_c(layer, ref, k, j):
        sl = rows(SLAB * rel(x, j), SLAB)
        out = [(g_gate.at[0, layer, sl, cols(WIN * k, WIN)], ref.at[k, sl, pl.ds(0, WIN)])]
        if UC:
            out.append((g_up.at[0, layer, sl, cols(UA + UC * k, UC)], ref.at[k, sl, pl.ds(WIN, UC)]))
        return out

    par_a, par_b, par_c = o_a.at[1 - c], o_b.at[1 - c], o_c.at[1 - c]
    there = {"a": o_a.at[c], "b": o_b.at[c], "c": o_c.at[c]}
    colours = {
        "c": (own_c, par_c, item_c, moves_c, z, "z", rc, SLAB, 32),
        "a": (own_a, par_a, item_a, moves_a, x, "x", ra, BLOCK, GROUP),
        "b": (own_b, par_b, item_b, moves_b, y, "y", rb, TALL, BLOCK),
    }

    locals_ = {}

    def load(src, dst, together):
        n = locals_.setdefault(together, len(locals_))
        pltpu.make_async_copy(src, dst, local.at[n]).start()

    def loaded(together, like):
        pltpu.make_async_copy(like, like, local.at[locals_[together]]).wait()

    sets = (((2, 0),), ((2, 2),), ((1, 2), (3, 0)), ((1, 0), (3, 2)), ((2, 1), (2, 3)), ((1, 3), (3, 1)), ((0, 0), (0, 2)), ((1, 1), (3, 3), (0, 1), (0, 3)))
    tail = (ALL, pl.ds(EDGE, LANES)), (ALL, pl.ds(UA, LANES))
    wide, tall = rows(SLAB * x + BLOCK * y, BLOCK), rows(TALL4 * x + TALL * y, TALL)
    state = [(w_gate.at[:, wide, :], wb_gate), (w_up.at[:, wide, :], wb_up), (w_down.at[:, tall, :], wb_down)]
    moments = ((m_gate, om_gate, m2_gate), (m_up, om_up, m2_up), (m_down, om_down, m2_down),
               (v_gate, ov_gate, v2_gate), (v_up, ov_up, v2_up), (v_down, ov_down, v2_down))
    state += [(src, dst) for src, dst, _ in moments]
    load(g_gate.at[(0, c, *tail[0])], own_a.at[tail[1]], "tail")
    for i, part in enumerate(sets):
        for dk, j in part:
            for n, (own, par, item, moves, k0, *_) in colours.items():
                for src, dst in moves(c, own, lax.rem(k0 + dk, 4), j):
                    load(src, dst, (n, i))
    for i, (src, dst) in enumerate(state):
        load(src, dst, ("state", i))
    at.barrier()
    net.start(g_gate.at[(0, 1 - c, *tail[0])], there["a"].at[tail[1]], at.partner, "da", "tail")
    for i, part in enumerate(sets):
        for dk, j in part:
            for n, (own, par, item, moves, k0, *_) in colours.items():
                for src, dst in moves(1 - c, there[n], lax.rem(k0 + dk, 4), j):
                    net.start(src, dst, at.partner, "d" + n, (n, i))
    here_is = set()

    def here_now(n, dk, j):
        i = [i for i, part in enumerate(sets) if (dk, j) in part][0]
        if (n, i) in here_is:
            return
        here_is.add((n, i))
        count = len(sets[i])
        if n == "a":
            like = own_a.at[pl.ds(0, BLOCK * count), pl.ds(0, UA)]
        elif n == "b":
            like = own_b.at[pl.ds(0, TALL * count), :]
        else:
            like = own_c.at[0, pl.ds(0, SLAB * count), :]
        loaded((n, i), like)
        net.arrived((n, i), like)

    def first(n):
        own, par, item, moves, k0, dim, r, height, step = colours[n]
        up, down = at.step(dim, 1), at.step(dim, 3)
        k2, kp, km = (lax.rem(k0 + d, 4) for d in (2, 1, 3))
        one, two = {}, {}
        if n == "a":
            like = own_a.at[:, pl.ds(0, LANES)]
            loaded("tail", like)
            net.arrived("tail", like)

        def opposite(j):
            here_now(n, 2, j)
            here = item(own, k2, j)
            vadd(here, (here, item(par, k2, j)), height, step)
            one[j] = net.start(here, r.at[j], up if j < 2 else down, "f" + n)

        def beside(dk, j, more):
            here_now(n, dk, j)
            if more:
                one[j].wait_recv()
            here = item(own, kp if dk == 1 else km, j)
            par_here = item(par, kp if dk == 1 else km, j)
            vadd(here, (here, par_here, r.at[j]) if more else (here, par_here), height, step)
            two[dk, j] = net.start(here, r.at[4 + j if dk == 1 else GROUP + j], up if dk == 1 else down, "f" + n)

        def mine(j):
            here_now(n, 0, j)
            two[1, j].wait_recv()
            two[3, j].wait_recv()
            here = item(own, k0, j)
            vadd(here, (here, item(par, k0, j), r.at[4 + j], r.at[GROUP + j]), height, step)

        opposite(0)
        yield
        opposite(2)
        yield
        beside(1, 2, False)
        yield
        beside(3, 0, False)
        yield
        beside(1, 0, True)
        yield
        beside(3, 2, True)
        yield
        opposite(1)
        yield
        opposite(3)
        yield
        beside(1, 3, False)
        yield
        beside(3, 1, False)
        yield
        mine(0)
        yield 0
        mine(2)
        yield 2
        beside(1, 1, True)
        yield
        beside(3, 3, True)
        yield
        mine(1)
        yield 1
        mine(3)
        yield 3

    def later(n, dim, block, halves, r1, r2, ready, step, done):
        up, down = at.step(dim, 1), at.step(dim, 3)
        for j in ready or (0, 2, 1, 3):
            if j == 0:
                a = net.start(halves(block(0), 0), halves(r1.at[0], 0, True), up, n)
                b = net.start(halves(block(0), 1), halves(r1.at[1], 1, True), down, n)
            if j == 2:
                net.start(halves(block(2), 1), halves(r2.at[0], 1), up, n, n)
            if j == 1:
                net.start(halves(block(1), 0), halves(r2.at[1], 0), down, n, n)
            if ready:
                yield
        a.wait_recv()
        here = halves(block(2), 0)
        vadd(here, (here, halves(r1.at[0], 0, True)), here.shape[0], GROUP)
        net.start(here, halves(r2.at[0], 0), up, n, n)
        yield
        b.wait_recv()
        here = halves(block(1), 1)
        vadd(here, (here, halves(r1.at[1], 1, True)), here.shape[0], GROUP)
        net.start(here, halves(r2.at[1], 1), down, n, n)
        yield
        net.arrived(n, r2)
        vadd(done, (block(3), r2.at[0], r2.at[1]), block(3).shape[0], step)

    def by_cols(w):
        def cut(ref, h, packed=False):
            return ref if packed else ref.at[:, pl.ds(h * w, w)]

        return cut

    def by_rows(n0, n1):
        def cut(ref, h, packed=False):
            return ref.at[pl.ds(0, (n0, n1)[h]), :] if packed else ref.at[pl.ds((0, n0)[h], (n0, n1)[h]), :]

        return cut

    def spread(n, full, blocks, height, snd, rcv):
        for k in range(GROUP):
            snd[k] = full[pl.ds(blocks * k, height), :].astype(BF)
        for zz, cc in at.group():
            s = 2 * zz + cc
            net.start(snd.at[s], rcv.at[at.g], at.dev(z=zz, c=cc), "s" + n, "s" + n)
        rcv[at.g] = snd[at.g]

    def prepare():
        for ref in (w2_gate, w2_up, w2_down, m2_gate, m2_up, m2_down, v2_gate, v2_up, v2_down):
            ref[...] = jnp.zeros(ref.shape, F32)
        for i, (_, dst) in enumerate(state):
            loaded(("state", i), dst)
        yield
        fw_wide[pl.ds(BLOCK, GROUP), :] = jnp.zeros((GROUP, FF), F32)
        fw_tall[pl.ds(TALL, GROUP), :] = jnp.zeros((GROUP, D), F32)
        for block, full, out, n, height in ((wb_gate, fw_wide, w2_gate, OWN_A, GROUP), (wb_up, fw_wide, w2_up, OWN_A, GROUP), (wb_down, fw_tall, w2_down, OWN_B, 32)):
            for layer in range(2):
                full[pl.ds(0, GROUP * n), :] = block[layer].astype(F32)
                for k in range(GROUP):

                    @pl.when(at.g == k)
                    def _():
                        out[layer] = full[pl.ds(n * k, height), :]

                yield
        for _, src, out in moments:
            for r in range(src.shape[0]):
                for layer in range(2):
                    out[layer, pl.ds(r, 1), :] = src[r, pl.ds(layer, 1), :]
            yield

    updated = []

    def finish():
        assert len(updated) == 3
        for _, out, src in moments:
            for r in range(out.shape[0]):
                for layer in range(2):
                    out[r, pl.ds(layer, 1), :] = src[layer, pl.ds(r, 1), :]
            yield

    gate, up_, down_ = (w2_gate, m2_gate, v2_gate), (w2_up, m2_up, v2_up), (w2_down, m2_down, v2_down)

    def update(which, start, layer, g, new, at_col):
        sl = (layer, ALL, pl.ds(start, g.shape[1]))
        w2, m2, v2 = which
        new_w, m2[sl], v2[sl] = adamw(w2[sl], m2[sl], v2[sl], g)
        new[layer, :, pl.ds(at_col, g.shape[1])] = new_w

    def summed(rcv, layer, sl):
        acc = rcv[layer, :, sl].astype(F32)
        for zz in range(1, 4):
            acc = acc + rcv[2 * zz + layer, :, sl].astype(F32)
        return acc.astype(BF).astype(F32)

    def pieces(start, end, most=896):
        return [(i, min(most, end - i)) for i in range(start, end, most)]

    def step_a():
        for layer in range(2):
            for i, n in pieces(0, UA):
                update(up_, i, layer, summed(rcv_a, layer, pl.ds(i, n)), new_a, i)
            update(gate, EDGE, layer, summed(rcv_a, layer, pl.ds(UA, LANES)), new_a, UA)

    def step_b():
        for layer in range(2):
            update(down_, 0, layer, summed(rcv_b, layer, pl.ds(0, D)), new_b, 0)

    def step_c():
        for layer in range(2):
            for zz in range(4):
                g = rcv_c[2 * zz + layer].astype(F32)
                update(gate, WIN * zz, layer, g[:, :WIN], new_c, WC * zz)
                if UC:
                    update(up_, UA + UC * zz, layer, g[:, WIN:], new_c, WC * zz + WIN)


    def over(n, ref):
        net.start(ref, ref, at.partner, "x" + n, "x" + n)

    def share(n, new, got):
        sl = (ALL, cols(WC * z, WC)) if n == "c" else (ALL, ALL)
        for zz, cc in at.group():
            there = (ALL, cols(WC * zz, WC)) if n == "c" else sl
            net.start(new.at[(cc, *there)], got.at[at.g], at.dev(z=zz, c=cc), "w" + n, "w" + n)
        got[at.g] = new[(c, *sl)]

    def build(n, blocks, got, full, out):
        net.arrived("w" + n, got.at[pl.ds(0, OTHERS)])
        for k in range(GROUP):
            full[pl.ds(blocks * k, blocks), :] = got[k].astype(F32)[:blocks]
        out[...] = full[pl.ds(0, GROUP * blocks), :].astype(BF)

    release = {}

    def small(n, dim, block, halves, brief=False):
        up, down = at.step(dim, 1), at.step(dim, 3)
        mine = block(3)
        m0 = net.start(halves(mine, 0), halves(mine, 0), up, n)
        p1 = net.start(halves(mine, 1), halves(mine, 1), down, n)
        m1 = net.start(halves(mine, 1), halves(mine, 1), up, n)
        p0 = net.start(halves(mine, 0), halves(mine, 0), down, n)
        yield 3
        m0.wait_recv()
        here = halves(block(1), 0)
        f0 = net.start(here, here, up, n)
        p1.wait_recv()
        here = halves(block(2), 1)
        f1 = net.start(here, here, down, n)
        yield
        m1.wait_recv()
        if not brief:
            yield 1
        p0.wait_recv()
        if not brief:
            yield 2
        f0.wait_recv()
        f1.wait_recv()
        if not brief:
            yield 0

    def large(n, dim, k0, item, ready):
        up, down = at.step(dim, 1), at.step(dim, 3)
        kp, km, k2 = (lax.rem(k0 + d, 4) for d in (1, 3, 2))
        fm, fp, order, held = {}, {}, [], []

        def flush():
            if held:
                j = held.pop(0)
                here = item(k0, j)
                fm[j] = net.start(here, here, up, "l" + n)
                fp[j] = net.start(here, here, down, "l" + n)
                over(n, here)
                order.append(j)

        release[n.upper()] = flush
        for j in ready:
            if j is not None:
                held.append(j)
            yield
        while held:
            flush()
            yield
        f2 = {}
        for j in order:
            fm[j].wait_recv()
            here = item(km, j)
            if j < 2:
                f2[j] = net.start(here, here, up, "l" + n)
            over(n, here)
            yield
            fp[j].wait_recv()
            here = item(kp, j)
            if j >= 2:
                f2[j] = net.start(here, here, down, "l" + n)
            over(n, here)
            yield
        for j in order:
            f2[j].wait_recv()
            over(n, item(k2, j))
            yield

    def colour_a():
        f_a[pl.ds(BLOCK, GROUP), :] = jnp.zeros((GROUP, WA), F32)
        yield from later("ma", "y", lambda j: item_a(own_a, x, j), by_cols(WA // 2), s1a, s2a, first("a"), GROUP, f_a)
        spread("a", f_a, OWN_A, GROUP, snd_a, rcv_a)
        yield
        net.arrived("sa", rcv_a.at[pl.ds(0, OTHERS)])
        step_a()
        updated.append("a")
        share("a", new_a, got_a)
        yield
        out = lambda k, j: item_a(o_a.at[c], k, j)
        build("a", OWN_A, got_a, f_a, out(x, 3))
        yield from large("a", "x", x, out, small("ga", "y", lambda j: out(x, j), by_cols(WA // 2)))

    def colour_b():
        f_b[pl.ds(TALL, GROUP), :] = jnp.zeros((GROUP, D), F32)
        yield from later("mb", "x", lambda j: item_b(own_b, y, j), by_rows(104, 96), s1b, s2b, first("b"), BLOCK, f_b)
        spread("b", f_b, OWN_B, 32, snd_b, rcv_b)
        yield
        net.arrived("sb", rcv_b.at[pl.ds(0, OTHERS)])
        step_b()
        updated.append("b")
        share("b", new_b, got_b)
        yield
        out = lambda k, j: item_b(o_b.at[c], k, j)
        build("b", OWN_B, got_b, f_b, out(y, 3))
        yield from large("b", "y", y, out, small("gb", "x", lambda j: out(y, j), by_rows(104, 96)))

    def colour_c():
        f_c[pl.ds(BLOCK, GROUP), :] = jnp.zeros((GROUP, WC), F32)
        yield from later("mc", "x", lambda j: item_c(own_c, z, j), by_rows(80, 80), s1c, s2c, first("c"), 32, item_c(own_c, z, 3))
        block = lambda j: own_c.at[z, rows(SLAB * x + BLOCK * rel(y, j), BLOCK), :]
        split = by_cols(WC // 2) if WC % 256 == 0 else by_rows(24, 16)
        yield from later("nc", "y", block, split, t1c, t2c, None, GROUP, f_c)
        spread("c", f_c, OWN_A, GROUP, snd_c, rcv_c)
        yield
        net.arrived("sc", rcv_c.at[pl.ds(0, OTHERS)])
        step_c()
        updated.append("c")
        share("c", new_c, got_c)
        yield
        out = lambda k, j: item_c(o_c.at[c], k, j)
        mine = lambda j: o_c.at[c, z, rows(SLAB * x + BLOCK * rel(y, j), BLOCK), :]
        build("c", OWN_A, got_c, f_c, mine(3))
        for _ in small("hc", "y", mine, split, True):
            yield
        yield from large("c", "z", z, out, small("gc", "x", lambda j: out(z, j), by_rows(80, 80)))

    interleave(PLAN, release, c=colour_c(), a=colour_a(), b=colour_b(), p=prepare(), f=finish())
    for n, (own, *_) in colours.items():
        net.arrived("x" + n, own)
    sizes = {"nc": own_c.at[0, pl.ds(0, 120), :], "hc": own_c.at[0, pl.ds(0, 120), :]}
    for n, (own, _, _, _, _, _, r, *_) in colours.items():
        sizes |= {"d" + n: own, "x" + n: own, "f" + n: r, "l" + n: r, "m" + n: r.at[pl.ds(0, 3)], "g" + n: r.at[pl.ds(0, 3)]}
    for n, rcv in (("a", rcv_a), ("b", rcv_b), ("c", rcv_c)):
        sizes |= {"s" + n: rcv.at[pl.ds(0, OTHERS)], "w" + n: rcv.at[pl.ds(0, OTHERS)]}
    net.drain(sizes)
    assert (net.n, len(net.groups), len(locals_)) == (RECV, SEND, LOCAL), (net.n, len(net.groups), len(locals_))


def write_kernel(a, b, c, *refs):
    small, (gate, up, down), outs, sem = refs[:6], refs[6:9], refs[9:15], refs[15]
    copies = [(b.at[l], down.at[l]) for l in range(2)]
    copies += [(a.at[l, :, pl.ds(0, UA)], up.at[l, :, pl.ds(0, UA)]) for l in range(2)]
    copies += [(c.at[l, k, :, pl.ds(0, WIN)], gate.at[l, :, pl.ds(WIN * k, WIN)]) for l in range(2) for k in range(4)]
    copies += [(a.at[l, :, pl.ds(UA, LANES)], gate.at[l, :, pl.ds(EDGE, LANES)]) for l in range(2)]
    if UC:
        copies += [(c.at[l, k, :, pl.ds(WIN, UC)], up.at[l, :, pl.ds(UA + UC * k, UC)]) for l in range(2) for k in range(4)]
    copies += list(zip(small, outs, strict=True))
    copies = [pltpu.make_async_copy(s, d, sem.at[i]) for i, (s, d) in enumerate(copies)]
    for copy in copies:
        copy.start()
    for copy in copies:
        copy.wait()


def spec(space, n):
    return [pl.BlockSpec(memory_space=space)] * n


def solution(mesh):
    def step(*arrays):
        terms, weights, m, v = (arrays[i : i + 3] for i in (0, 3, 6, 9))
        turn = lambda one: jnp.transpose(one, (1, 0, 2))
        moments = [turn(one) for one in (*m, *v)]
        own_rows = [(2, GROUP, FF), (2, GROUP, FF), (2, 32, D)]
        blocks = [(GROUP, GROUP, WA), (GROUP, 32, D), (GROUP, GROUP, WC)]
        results = pl.pallas_call(
            step_kernel,
            out_shape=[
                VMEM((2, D, WA), BF),
                VMEM((2, FF, D), BF),
                VMEM((2, 4, D, WC), BF),
                *[VMEM(one.shape, F32) for one in moments],
            ],
            in_specs=spec(HBM, 12),
            out_specs=spec(VMEM, 9),
            scratch_shapes=[
                VMEM((D, WA), BF),
                VMEM((FF, D), BF),
                VMEM((4, D, WC), BF),
                *[VMEM((12, *s), BF) for s in ((BLOCK, WA), (TALL, D), (SLAB, WC))],
                VMEM((2, BLOCK, WA // 2), BF),
                VMEM((2, BLOCK, WA), BF),
                VMEM((2, 104, D), BF),
                VMEM((2, TALL, D), BF),
                VMEM((2, 80, WC), BF),
                VMEM((2, SLAB, WC), BF),
                VMEM((2, BLOCK, WC // 2) if WC % 256 == 0 else (2, 24, WC), BF),
                VMEM((2, BLOCK, WC), BF),
                VMEM((BLOCK_PAD, WA), F32),
                VMEM((TALL_PAD, D), F32),
                VMEM((BLOCK_PAD, WC), F32),
                *[VMEM(s, BF) for s in blocks] * 2,
                VMEM((2, GROUP, WA), BF),
                VMEM((2, 32, D), BF),
                VMEM((2, GROUP, 4 * WC), BF),
                *[VMEM(s, BF) for s in blocks],
                VMEM((2, BLOCK, FF), BF),
                VMEM((2, BLOCK, FF), BF),
                VMEM((2, TALL, D), BF),
                VMEM((BLOCK_PAD, FF), F32),
                VMEM((TALL_PAD, D), F32),
                *[VMEM(s, F32) for s in own_rows] * 3,
                pltpu.SemaphoreType.DMA((SEND,)),
                pltpu.SemaphoreType.DMA((RECV,)),
                pltpu.SemaphoreType.DMA((LOCAL,)),
            ],
            compiler_params=pltpu.CompilerParams(collective_id=0, has_side_effects=True, vmem_limit_bytes=34 * 2**20),
            name="step",
        )(*terms, *weights, *moments)
        done = pl.pallas_call(
            write_kernel,
            out_shape=[jax.ShapeDtypeStruct(w.shape, BF) for w in weights] + [jax.ShapeDtypeStruct(one.shape, F32) for one in moments],
            in_specs=spec(VMEM, 9),
            out_specs=spec(HBM, 9),
            scratch_shapes=[pltpu.SemaphoreType.DMA((30,))],
            compiler_params=pltpu.CompilerParams(vmem_limit_bytes=2**20),
            name="write",
        )(*results)
        return (*done[:3], *(turn(one) for one in done[3:]))

    all_of, cut = P(None, None, None), P(None, "dp", None)
    return jax.shard_map(
        step,
        mesh=mesh,
        in_specs=(P(("rep", "dp"), None, None, None),) * 3 + (all_of,) * 3 + (cut,) * 6,
        out_specs=(P("rep", None, None),) * 3 + (P("rep", "dp", None),) * 6,
        check_vma=False,
    )
```

```python
import jax
import jax.numpy as jnp
from jax import lax
from jax.experimental import pallas as pl
from jax.experimental.pallas import tpu as pltpu
from jax.sharding import PartitionSpec as P

ALL = slice(None)
BF, F32 = jnp.bfloat16, jnp.float32
D, FF, LANES, GROUP, OTHERS = 640, 3200, 128, 8, 7
OWN_A, OWN_B = 5, 25
BLOCK, SLAB, TALL, TALL4 = 40, 160, 200, 800
BLOCK_PAD, TALL_PAD = 48, 208
WIN, EDGE = 768, 3072
SHARE = 1
UC = 128 * SHARE
UA = 3200 - 4 * UC
WA = UA + 128
WC = 768 + UC
PACK_A, PACK_B, PACK_C = 112, 128, 40
PLAN = "cab" * 10 + "pppppppp" + "cab" * 2 + "pppppppppp" + "acb" * 2 + "aaaa" + "cbcb" + "cbcb"
PLAN += "aacb" + "aA" + "cb" + "cb" + "cc" + "C" + "abB" + "abc" + "ABC" + "abc" + "ABC" + "abc" + "ABC"
PLAN += "f" * 9
SEND, RECV, LOCAL = 26, 120, 34
OFF = (2, 3, 1, 0)
HBM = pltpu.MemorySpace.HBM
VMEM = pltpu.MemorySpace.VMEM


def adamw(w, m, v, g):
    m = 0.9 * m + 0.1 * g
    v = 0.95 * v + 0.05 * g * g
    step = m * lax.rsqrt(v + 1e-8) + 0.1 * w
    return (w - 0.02 * step).astype(jnp.bfloat16), m, v


class Place:
    def __init__(self):
        me = lax.axis_index("dp")
        self.c = lax.rem(me, 2)
        self.z = lax.rem(me // 2, 4)
        self.y = lax.rem(me // GROUP, 4)
        self.x = me // 32
        self.g = lax.rem(me, GROUP)
        self.partner = self.dev(c=1 - self.c)

    def dev(self, x=None, y=None, z=None, c=None):
        x = self.x if x is None else x
        y = self.y if y is None else y
        z = self.z if z is None else z
        c = self.c if c is None else c
        return {"dp": ((x * 4 + y) * 4 + z) * 2 + c}

    def step(self, dim, by):
        return self.dev(**{dim: lax.rem(getattr(self, dim) + by, 4)})

    def group(self):
        out = [(self.z, 1 - self.c)]
        for dz in (1, 2, 3):
            zz = lax.rem(self.z + dz, 4)
            out += [(zz, self.c), (zz, 1 - self.c)]
        return out

    def barrier(self):
        sem = pltpu.get_barrier_semaphore()
        peers = [self.dev(z=z, c=c) for z, c in self.group()]
        peers += [self.step(d, by) for d in ("x", "y") for by in (1, 3)]
        for peer in peers:
            pl.semaphore_signal(sem, inc=1, device_id=peer, device_id_type=pl.DeviceIdType.MESH)
        pl.semaphore_wait(sem, len(peers))


class Sender:
    def __init__(self, send, recv):
        self.send, self.recv, self.n, self.groups, self.shared = send, recv, 0, {}, {}

    def start(self, src, dst, device, group, together=None):
        mine = self.groups.setdefault(group, len(self.groups))
        if together is None or together not in self.shared:
            got = self.n
            self.n += 1
            if together is not None:
                self.shared[together] = got
        else:
            got = self.shared[together]
        copy = pltpu.make_async_remote_copy(
            src_ref=src,
            dst_ref=dst,
            send_sem=self.send.at[mine],
            recv_sem=self.recv.at[got],
            device_id=device,
            device_id_type=pl.DeviceIdType.MESH,
        )
        copy.start()
        return copy

    def arrived(self, together, like):
        pltpu.make_async_copy(like, like, self.recv.at[self.shared[together]]).wait()

    def drain(self, sizes):
        for group, n in self.groups.items():
            like = sizes[group]
            pltpu.make_async_copy(like, like, self.send.at[n]).wait()


def rows(start, n):
    return pl.ds(pl.multiple_of(start, GROUP), n)


def total(refs, sl):
    acc = refs[0][sl].astype(F32)
    for r in refs[1:]:
        acc = acc + r[sl].astype(F32)
    return acc


def vadd(dst, refs, n, step):
    def body(i, carry):
        sl = (rows(i * step, step), ALL)
        dst[sl] = total(refs, sl).astype(dst.dtype)
        return carry

    lax.fori_loop(0, n // step, body, 0)


def interleave(plan, release, **programs):
    live = dict(programs)

    def advance(n):
        try:
            next(live[n])
        except StopIteration:
            del live[n]

    for n in plan:
        if n in release:
            release[n]()
        elif n in live:
            advance(n)
    while live:
        for n in list(live):
            advance(n)


def step_kernel(g_gate, g_up, g_down, w_gate, w_up, w_down, m_gate, m_up, m_down, v_gate, v_up, v_down,
                o_a, o_b, o_c, om_gate, om_up, om_down, ov_gate, ov_up, ov_down,
                own_a, own_b, own_c, ra, rb, rc, s1a, s2a, s1b, s2b, s1c, s2c, tc, f_a, f_b, f_c,
                snd_a, snd_b, snd_c, rcv_a, rcv_b, rcv_c, new_a, new_b, new_c, got_a, got_b, got_c,
                wb_gate, wb_up, wb_down, fw_wide, fw_tall, pk_a, pk_b, pk_c, sw_a, sw_b, sw_c, sm_a, sm_b, sm_c, sv_a, sv_b, sv_c, w2_gate, w2_up, w2_down, m2_gate, m2_up, m2_down, v2_gate, v2_up, v2_down,
                send, recv, local):
    at = Place()
    x, y, z, c = at.x, at.y, at.z, at.c
    net = Sender(send, recv)
    loads = [0]
    rel = lambda base, j: lax.rem(base + OFF[j], 4)
    cols = lambda start, n: pl.ds(pl.multiple_of(start, LANES), n)

    def item_a(ref, k, j):
        return ref.at[rows(SLAB * k + BLOCK * rel(y, j), BLOCK), :]

    def item_b(ref, k, j):
        return ref.at[rows(TALL * k + TALL4 * rel(x, j), TALL), :]

    def item_c(ref, k, j):
        return ref.at[k, rows(SLAB * rel(x, j), SLAB), :]

    def moves_a(layer, ref, k, j):
        sl = rows(SLAB * k + BLOCK * rel(y, j), BLOCK)
        return [(g_up.at[0, layer, sl, pl.ds(0, UA)], ref.at[sl, pl.ds(0, UA)])]

    def moves_b(layer, ref, k, j):
        return [(g_down.at[0, layer, rows(TALL * k + TALL4 * rel(x, j), TALL), :], item_b(ref, k, j))]

    def moves_c(layer, ref, k, j):
        sl = rows(SLAB * rel(x, j), SLAB)
        out = [(g_gate.at[0, layer, sl, cols(WIN * k, WIN)], ref.at[k, sl, pl.ds(0, WIN)])]
        if UC:
            out.append((g_up.at[0, layer, sl, cols(UA + UC * k, UC)], ref.at[k, sl, pl.ds(WIN, UC)]))
        return out

    par_a, par_b, par_c = o_a.at[1 - c], o_b.at[1 - c], o_c.at[1 - c]
    there = {"a": o_a.at[c], "b": o_b.at[c], "c": o_c.at[c]}
    colours = {
        "c": (own_c, par_c, item_c, moves_c, z, "z", rc, SLAB, 32),
        "a": (own_a, par_a, item_a, moves_a, x, "x", ra, BLOCK, GROUP),
        "b": (own_b, par_b, item_b, moves_b, y, "y", rb, TALL, BLOCK),
    }

    locals_ = {}

    def load(src, dst, together):
        n = locals_.setdefault(together, len(locals_))
        pltpu.make_async_copy(src, dst, local.at[n]).start()

    def loaded(together, like):
        pltpu.make_async_copy(like, like, local.at[locals_[together]]).wait()

    sets = (((2, 0),), ((2, 2),), ((1, 2), (3, 0)), ((1, 0), (3, 2)), ((2, 1), (2, 3)), ((1, 3), (3, 1)), ((0, 0), (0, 2)), ((1, 1), (3, 3), (0, 1), (0, 3)))
    tail = (ALL, pl.ds(EDGE, LANES)), (ALL, pl.ds(UA, LANES))
    wide, tall = rows(SLAB * x + BLOCK * y, BLOCK), rows(TALL4 * x + TALL * y, TALL)
    state = [(w_gate.at[:, wide, :], wb_gate), (w_up.at[:, wide, :], wb_up), (w_down.at[:, tall, :], wb_down)]
    moments = ((m_gate, om_gate, m2_gate), (m_up, om_up, m2_up), (m_down, om_down, m2_down),
               (v_gate, ov_gate, v2_gate), (v_up, ov_up, v2_up), (v_down, ov_down, v2_down))
    state += [(src, dst) for src, dst, _ in moments]
    load(g_gate.at[(0, c, *tail[0])], own_a.at[tail[1]], "tail")
    for i, part in enumerate(sets):
        for dk, j in part:
            for n, (own, par, item, moves, k0, *_) in colours.items():
                for src, dst in moves(c, own, lax.rem(k0 + dk, 4), j):
                    load(src, dst, (n, i))
    for i, (src, dst) in enumerate(state):
        load(src, dst, ("state", i))
    at.barrier()
    net.start(g_gate.at[(0, 1 - c, *tail[0])], there["a"].at[tail[1]], at.partner, "da", "tail")
    for i, part in enumerate(sets):
        for dk, j in part:
            for n, (own, par, item, moves, k0, *_) in colours.items():
                for src, dst in moves(1 - c, there[n], lax.rem(k0 + dk, 4), j):
                    net.start(src, dst, at.partner, "d" + n, (n, i))
    here_is = set()

    def here_now(n, dk, j):
        i = [i for i, part in enumerate(sets) if (dk, j) in part][0]
        if (n, i) in here_is:
            return
        here_is.add((n, i))
        count = len(sets[i])
        if n == "a":
            like = own_a.at[pl.ds(0, BLOCK * count), pl.ds(0, UA)]
        elif n == "b":
            like = own_b.at[pl.ds(0, TALL * count), :]
        else:
            like = own_c.at[0, pl.ds(0, SLAB * count), :]
        loaded((n, i), like)
        net.arrived((n, i), like)

    def first(n):
        own, par, item, moves, k0, dim, r, height, step = colours[n]
        up, down = at.step(dim, 1), at.step(dim, 3)
        k2, kp, km = (lax.rem(k0 + d, 4) for d in (2, 1, 3))
        one = {}
        if n == "a":
            like = own_a.at[:, pl.ds(0, LANES)]
            loaded("tail", like)
            net.arrived("tail", like)

        def opposite(j):
            here_now(n, 2, j)
            here = item(own, k2, j)
            vadd(here, (here, item(par, k2, j)), height, step)
            one[j] = net.start(here, r.at[j], up if j < 2 else down, "f" + n)

        def beside(dk, j, more):
            here_now(n, dk, j)
            if more:
                one[j].wait_recv()
            here = item(own, kp if dk == 1 else km, j)
            par_here = item(par, kp if dk == 1 else km, j)
            vadd(here, (here, par_here, r.at[j]) if more else (here, par_here), height, step)
            net.start(here, r.at[4 + j if dk == 1 else GROUP + j], up if dk == 1 else down, "f" + n, (n, "two", j))

        def mine(j):
            here_now(n, 0, j)
            net.arrived((n, "two", j), r.at[pl.ds(0, 2)])
            here = item(own, k0, j)
            vadd(here, (here, item(par, k0, j), r.at[4 + j], r.at[GROUP + j]), height, step)

        opposite(0)
        yield
        opposite(2)
        yield
        beside(1, 2, False)
        yield
        beside(3, 0, False)
        yield
        beside(1, 0, True)
        yield
        beside(3, 2, True)
        yield
        opposite(1)
        yield
        opposite(3)
        yield
        beside(1, 3, False)
        yield
        beside(3, 1, False)
        yield
        mine(0)
        yield 0
        mine(2)
        yield 2
        beside(1, 1, True)
        yield
        beside(3, 3, True)
        yield
        mine(1)
        yield 1
        mine(3)
        yield 3

    def later(n, dim, block, halves, r1, r2, ready, hold, step, done):
        up, down = at.step(dim, 1), at.step(dim, 3)
        waiting = []
        for i, chunk in enumerate(ready):
            if chunk is not None:
                waiting.append(chunk)
            while waiting and i >= hold:
                j = waiting.pop(0)
                if j == 0:
                    a = net.start(halves(block(0), 0), halves(r1.at[0], 0, True), up, n)
                    b = net.start(halves(block(0), 1), halves(r1.at[1], 1, True), down, n)
                if j == 2:
                    net.start(halves(block(2), 1), halves(r2.at[0], 1), up, n, n)
                if j == 1:
                    net.start(halves(block(1), 0), halves(r2.at[1], 0), down, n, n)
            yield
        a.wait_recv()
        here = halves(block(2), 0)
        vadd(here, (here, halves(r1.at[0], 0, True)), here.shape[0], GROUP)
        net.start(here, halves(r2.at[0], 0), up, n, n)
        yield
        b.wait_recv()
        here = halves(block(1), 1)
        vadd(here, (here, halves(r1.at[1], 1, True)), here.shape[0], GROUP)
        net.start(here, halves(r2.at[1], 1), down, n, n)
        yield
        net.arrived(n, r2)
        vadd(done, (block(3), r2.at[0], r2.at[1]), block(3).shape[0], step)

    def by_cols(w):
        def cut(ref, h, packed=False):
            return ref if packed else ref.at[:, pl.ds(h * w, w)]

        return cut

    def by_rows(n0, n1):
        def cut(ref, h, packed=False):
            return ref.at[pl.ds(0, (n0, n1)[h]), :] if packed else ref.at[pl.ds((0, n0)[h], (n0, n1)[h]), :]

        return cut

    def spread(n, full, blocks, packed, snd, rcv):
        for k in range(GROUP):
            for t in range(full.shape[1] // LANES):
                packed[k, pl.ds(blocks * t, blocks), :] = full[pl.ds(blocks * k, blocks), pl.ds(LANES * t, LANES)]
            snd[k] = packed[k].astype(BF)
        for zz, cc in at.group():
            s = 2 * zz + cc
            net.start(snd.at[s], rcv.at[at.g], at.dev(z=zz, c=cc), "s" + n, "s" + n)
        rcv[at.g] = snd[at.g]

    def prepare():
        for ref in (sw_a, sw_b, sw_c, sm_a, sm_b, sm_c, sv_a, sv_b, sv_c):
            ref[...] = jnp.zeros(ref.shape, F32)
        for i, (_, dst) in enumerate(state):
            loaded(("state", i), dst)
        yield
        fw_wide[pl.ds(BLOCK, GROUP), :] = jnp.zeros((GROUP, FF), F32)
        fw_tall[pl.ds(TALL, GROUP), :] = jnp.zeros((GROUP, D), F32)
        for block, full, out, n, height in ((wb_gate, fw_wide, w2_gate, OWN_A, GROUP), (wb_up, fw_wide, w2_up, OWN_A, GROUP), (wb_down, fw_tall, w2_down, OWN_B, 32)):
            for layer in range(2):
                full[pl.ds(0, GROUP * n), :] = block[layer].astype(F32)
                for k in range(GROUP):

                    @pl.when(at.g == k)
                    def _():
                        out[layer] = full[pl.ds(n * k, height), :]

                yield
        for _, src, out in moments:
            for r in range(src.shape[0]):
                for layer in range(2):
                    out[layer, pl.ds(r, 1), :] = src[r, pl.ds(layer, 1), :]
            yield
        for which in kept:
            for to, here, there in tiles(*which):
                here[to] = there[...]
            yield

    def tiles(wide_gate, wide_up, tall, in_a, in_b, in_c):
        for layer in range(2):
            for t in range(OWN_B):
                piece = (layer, pl.ds(0, OWN_A), pl.ds(LANES * t, LANES))
                if t < 24:
                    yield (layer, t // 6, pl.ds(OWN_A * (t % 6), OWN_A)), in_c, wide_gate.at[piece]
                else:
                    yield (layer, pl.ds(OWN_A * (UA // LANES), OWN_A)), in_a, wide_gate.at[piece]
                if t < UA // LANES:
                    yield (layer, pl.ds(OWN_A * t, OWN_A)), in_a, wide_up.at[piece]
                else:
                    yield (layer, (t - UA // LANES) // SHARE, pl.ds(OWN_A * (6 + (t - UA // LANES) % SHARE), OWN_A)), in_c, wide_up.at[piece]
            for t in range(OWN_A):
                yield (layer, pl.ds(OWN_B * t, OWN_B)), in_b, tall.at[layer, pl.ds(0, OWN_B), pl.ds(LANES * t, LANES)]

    kept = (
        (w2_gate, w2_up, w2_down, sw_a, sw_b, sw_c),
        (m2_gate, m2_up, m2_down, sm_a, sm_b, sm_c),
        (v2_gate, v2_up, v2_down, sv_a, sv_b, sv_c),
    )
    updated = []

    def finish():
        assert len(updated) == 3
        for which in kept[1:]:
            for to, here, there in tiles(*which):
                there[...] = here[to]
            yield
        for _, out, src in moments:
            for r in range(out.shape[0]):
                for layer in range(2):
                    out[r, pl.ds(layer, 1), :] = src[layer, pl.ds(r, 1), :]
            yield

    def update(state, at_, g, new):
        w2, m2, v2 = state
        new[at_], m2[at_], v2[at_] = adamw(w2[at_], m2[at_], v2[at_], g)

    def summed(rcv, layer):
        acc = rcv[layer].astype(F32)
        for zz in range(1, 4):
            acc = acc + rcv[2 * zz + layer].astype(F32)
        return acc.astype(BF).astype(F32)

    def step_a():
        for layer in range(2):
            update((sw_a, sm_a, sv_a), layer, summed(rcv_a, layer), new_a)

    def step_b():
        for layer in range(2):
            update((sw_b, sm_b, sv_b), layer, summed(rcv_b, layer), new_b)

    def step_c():
        for layer in range(2):
            for zz in range(4):
                update((sw_c, sm_c, sv_c), (layer, zz), rcv_c[2 * zz + layer].astype(F32), new_c)

    def over(n, ref):
        net.start(ref, ref, at.partner, "x" + n, "x" + n)

    def share(n, new, got):
        for zz, cc in at.group():
            one = new.at[cc, zz] if n == "c" else new.at[cc]
            net.start(one, got.at[at.g], at.dev(z=zz, c=cc), "w" + n, "w" + n)
        got[at.g] = new[c, z] if n == "c" else new[c]

    def build(n, blocks, got, full, out):
        net.arrived("w" + n, got.at[pl.ds(0, OTHERS)])
        for k in range(GROUP):
            one = got[k].astype(F32)
            for t in range(full.shape[1] // LANES):
                full[pl.ds(blocks * k, blocks), pl.ds(LANES * t, LANES)] = one[blocks * t : blocks * (t + 1)]
        out[...] = full[pl.ds(0, GROUP * blocks), :].astype(BF)

    release = {}

    def small(n, dim, block, halves):
        up, down = at.step(dim, 1), at.step(dim, 3)
        mine = block(3)
        m0 = net.start(halves(mine, 0), halves(mine, 0), up, n)
        p1 = net.start(halves(mine, 1), halves(mine, 1), down, n)
        m1 = net.start(halves(mine, 1), halves(mine, 1), up, n)
        p0 = net.start(halves(mine, 0), halves(mine, 0), down, n)
        yield 3
        m0.wait_recv()
        here = halves(block(1), 0)
        net.start(here, here, up, n, n)
        p1.wait_recv()
        here = halves(block(2), 1)
        net.start(here, here, down, n, n)
        yield
        m1.wait_recv()
        yield 1
        p0.wait_recv()
        yield 2
        net.arrived(n, mine)
        yield 0

    def large(n, dim, k0, item, ready):
        up, down = at.step(dim, 1), at.step(dim, 3)
        kp, km, k2 = (lax.rem(k0 + d, 4) for d in (1, 3, 2))
        fm, fp, order, held = {}, {}, [], []

        def flush():
            if held:
                j = held.pop(0)
                here = item(k0, j)
                fm[j] = net.start(here, here, up, "l" + n)
                fp[j] = net.start(here, here, down, "l" + n)
                over(n, here)
                order.append(j)

        release[n.upper()] = flush
        for j in ready:
            if j is not None:
                held.append(j)
            yield
        while held:
            flush()
            yield
        f2 = {}
        for j in order:
            fm[j].wait_recv()
            here = item(km, j)
            if j < 2:
                f2[j] = net.start(here, here, up, "l" + n)
            over(n, here)
            yield
            fp[j].wait_recv()
            here = item(kp, j)
            if j >= 2:
                f2[j] = net.start(here, here, down, "l" + n)
            over(n, here)
            yield
        for j in order:
            f2[j].wait_recv()
            over(n, item(k2, j))
            yield

    def colour_a():
        pk_a[...] = jnp.zeros(pk_a.shape, F32)
        yield from later("ma", "y", lambda j: item_a(own_a, x, j), by_cols(WA // 2), s1a, s2a, first("a"), 0, GROUP, f_a)
        spread("a", f_a, OWN_A, pk_a, snd_a, rcv_a)
        yield
        net.arrived("sa", rcv_a.at[pl.ds(0, OTHERS)])
        step_a()
        updated.append("a")
        share("a", new_a, got_a)
        yield
        out = lambda k, j: item_a(o_a.at[c], k, j)
        build("a", OWN_A, got_a, f_a, out(x, 3))
        yield from large("a", "x", x, out, small("ga", "y", lambda j: out(x, j), by_cols(WA // 2)))

    def colour_b():
        pk_b[...] = jnp.zeros(pk_b.shape, F32)
        yield from later("mb", "x", lambda j: item_b(own_b, y, j), by_rows(104, 96), s1b, s2b, first("b"), 13, BLOCK, f_b)
        spread("b", f_b, OWN_B, pk_b, snd_b, rcv_b)
        yield
        net.arrived("sb", rcv_b.at[pl.ds(0, OTHERS)])
        step_b()
        updated.append("b")
        share("b", new_b, got_b)
        yield
        out = lambda k, j: item_b(o_b.at[c], k, j)
        build("b", OWN_B, got_b, f_b, out(y, 3))
        yield from large("b", "y", y, out, small("gb", "x", lambda j: out(y, j), by_rows(104, 96)))

    def colour_c():
        pk_c[...] = jnp.zeros(pk_c.shape, F32)
        yield from later("mc", "x", lambda j: item_c(own_c, z, j), by_rows(80, 80), s1c, s2c, first("c"), 13, 32, item_c(own_c, z, 3))
        part = lambda ref, yy: ref.at[z, rows(SLAB * x + BLOCK * yy, BLOCK), :]
        for d in (1, 2, 3):
            yy = lax.rem(y + d, 4)
            net.start(part(own_c, yy), tc.at[d - 1], at.step("y", d), "nc", "nc")
        yield
        net.arrived("nc", tc)
        vadd(f_c, (part(own_c, y), *(tc.at[d] for d in range(3))), BLOCK, GROUP)
        spread("c", f_c, OWN_A, pk_c, snd_c, rcv_c)
        yield
        net.arrived("sc", rcv_c.at[pl.ds(0, OTHERS)])
        step_c()
        updated.append("c")
        share("c", new_c, got_c)
        yield
        out = lambda k, j: item_c(o_c.at[c], k, j)
        mine = part(o_c.at[c], y)
        build("c", OWN_A, got_c, f_c, mine)
        for d in (1, 3, 2):
            net.start(mine, mine, at.step("y", d), "hc", "hc")
        yield
        net.arrived("hc", tc)
        yield from large("c", "z", z, out, small("gc", "x", lambda j: out(z, j), by_rows(80, 80)))

    interleave(PLAN, release, c=colour_c(), a=colour_a(), b=colour_b(), p=prepare(), f=finish())
    for n, (own, *_) in colours.items():
        net.arrived("x" + n, own)
    sizes = {"nc": tc, "hc": tc}
    for n, (own, _, _, _, _, _, r, *_) in colours.items():
        sizes |= {"d" + n: own, "x" + n: own, "f" + n: r, "l" + n: r, "m" + n: r.at[pl.ds(0, 3)], "g" + n: r.at[pl.ds(0, 3)]}
    for n, rcv in (("a", rcv_a), ("b", rcv_b), ("c", rcv_c)):
        sizes |= {"s" + n: rcv.at[pl.ds(0, OTHERS)], "w" + n: rcv.at[pl.ds(0, OTHERS)]}
    net.drain(sizes)
    assert (net.n, len(net.groups), len(locals_)) == (RECV, SEND, LOCAL), (net.n, len(net.groups), len(locals_))


def write_kernel(a, b, c, *refs):
    small, (gate, up, down), outs, sem = refs[:6], refs[6:9], refs[9:15], refs[15]
    copies = [(b.at[l], down.at[l]) for l in range(2)]
    copies += [(a.at[l, :, pl.ds(0, UA)], up.at[l, :, pl.ds(0, UA)]) for l in range(2)]
    copies += [(c.at[l, k, :, pl.ds(0, WIN)], gate.at[l, :, pl.ds(WIN * k, WIN)]) for l in range(2) for k in range(4)]
    copies += [(a.at[l, :, pl.ds(UA, LANES)], gate.at[l, :, pl.ds(EDGE, LANES)]) for l in range(2)]
    if UC:
        copies += [(c.at[l, k, :, pl.ds(WIN, UC)], up.at[l, :, pl.ds(UA + UC * k, UC)]) for l in range(2) for k in range(4)]
    copies += list(zip(small, outs, strict=True))
    for src, dst in copies:
        pltpu.make_async_copy(src, dst, sem).start()
    for out in (gate, up, down, *outs):
        pltpu.make_async_copy(out, out, sem).wait()


def spec(space, n):
    return [pl.BlockSpec(memory_space=space)] * n


def solution(mesh):
    def step(*arrays):
        terms, weights, m, v = (arrays[i : i + 3] for i in (0, 3, 6, 9))
        turn = lambda one: jnp.transpose(one, (1, 0, 2))
        moments = [turn(one) for one in (*m, *v)]
        own_rows = [(2, GROUP, FF), (2, GROUP, FF), (2, 32, D)]
        blocks = [(GROUP, PACK_A, LANES), (GROUP, PACK_B, LANES), (GROUP, PACK_C, LANES)]
        states = [(2, PACK_A, LANES), (2, PACK_B, LANES), (2, 4, PACK_C, LANES)]
        results = pl.pallas_call(
            step_kernel,
            out_shape=[
                VMEM((2, D, WA), BF),
                VMEM((2, FF, D), BF),
                VMEM((2, 4, D, WC), BF),
                *[VMEM(one.shape, F32) for one in moments],
            ],
            in_specs=spec(HBM, 12),
            out_specs=spec(VMEM, 9),
            scratch_shapes=[
                VMEM((D, WA), BF),
                VMEM((FF, D), BF),
                VMEM((4, D, WC), BF),
                *[VMEM((12, *s), BF) for s in ((BLOCK, WA), (TALL, D), (SLAB, WC))],
                VMEM((2, BLOCK, WA // 2), BF),
                VMEM((2, BLOCK, WA), BF),
                VMEM((2, 104, D), BF),
                VMEM((2, TALL, D), BF),
                VMEM((2, 80, WC), BF),
                VMEM((2, SLAB, WC), BF),
                VMEM((3, BLOCK, WC), BF),
                VMEM((BLOCK_PAD, WA), F32),
                VMEM((TALL_PAD, D), F32),
                VMEM((BLOCK_PAD, WC), F32),
                *[VMEM(s, BF) for s in blocks] * 2,
                *[VMEM(s, BF) for s in states],
                *[VMEM(s, BF) for s in blocks],
                VMEM((2, BLOCK, FF), BF),
                VMEM((2, BLOCK, FF), BF),
                VMEM((2, TALL, D), BF),
                VMEM((BLOCK_PAD, FF), F32),
                VMEM((TALL_PAD, D), F32),
                *[VMEM(s, F32) for s in blocks],
                *[VMEM(s, F32) for s in states] * 3,
                *[VMEM(s, F32) for s in own_rows] * 3,
                pltpu.SemaphoreType.DMA((SEND,)),
                pltpu.SemaphoreType.DMA((RECV,)),
                pltpu.SemaphoreType.DMA((LOCAL,)),
            ],
            compiler_params=pltpu.CompilerParams(collective_id=0, has_side_effects=True, vmem_limit_bytes=36 * 2**20),
            name="step",
        )(*terms, *weights, *moments)
        done = pl.pallas_call(
            write_kernel,
            out_shape=[jax.ShapeDtypeStruct(w.shape, BF) for w in weights] + [jax.ShapeDtypeStruct(one.shape, F32) for one in moments],
            in_specs=spec(VMEM, 9),
            out_specs=spec(HBM, 9),
            scratch_shapes=[pltpu.SemaphoreType.DMA],
            compiler_params=pltpu.CompilerParams(vmem_limit_bytes=2**20),
            name="write",
        )(*results)
        return (*done[:3], *(turn(one) for one in done[3:]))

    all_of, cut = P(None, None, None), P(None, "dp", None)
    return jax.shard_map(
        step,
        mesh=mesh,
        in_specs=(P(("rep", "dp"), None, None, None),) * 3 + (all_of,) * 3 + (cut,) * 6,
        out_specs=(P("rep", None, None),) * 3 + (P("rep", "dp", None),) * 6,
        check_vma=False,
    )
```

```python
import jax
import jax.numpy as jnp
from jax import lax
from jax.experimental import pallas as pl
from jax.experimental.pallas import tpu as pltpu
from jax.sharding import PartitionSpec as P

ALL = slice(None)
BF, F32 = jnp.bfloat16, jnp.float32
D, FF, LANES, GROUP, OTHERS = 640, 3200, 128, 8, 7
OWN_A, OWN_B = 5, 25
BLOCK, SLAB, TALL, TALL4 = 40, 160, 200, 800
BLOCK_PAD, TALL_PAD = 48, 208
WIN, EDGE = 768, 3072
SHARE = 1
UC = 128 * SHARE
UA = 3200 - 4 * UC
WA = UA + 128
WC = 768 + UC
PACK_A, PACK_B, PACK_C = 112, 128, 40
PLAN = (
    "cabcabcabcabcabcabcabcabcabcabppppppppcabcabpppp"
    "ppppppacbacbaaaaccccbbbbacacaAbcabaAccCbBccCcCbb"
    "BbBcCbBaAaAAfffffffff"
)
SEND, RECV, LOCAL = 26, 120, 34
OFF = (2, 3, 1, 0)
HBM = pltpu.MemorySpace.HBM
VMEM = pltpu.MemorySpace.VMEM


def adamw(w, m, v, g):
    m = 0.9 * m + 0.1 * g
    v = 0.95 * v + 0.05 * g * g
    step = m * lax.rsqrt(v + 1e-8) + 0.1 * w
    return (w - 0.02 * step).astype(jnp.bfloat16), m, v


class Place:
    def __init__(self):
        me = lax.axis_index("dp")
        self.c = lax.rem(me, 2)
        self.z = lax.rem(me // 2, 4)
        self.y = lax.rem(me // GROUP, 4)
        self.x = me // 32
        self.g = lax.rem(me, GROUP)
        self.partner = self.dev(c=1 - self.c)

    def dev(self, x=None, y=None, z=None, c=None):
        x = self.x if x is None else x
        y = self.y if y is None else y
        z = self.z if z is None else z
        c = self.c if c is None else c
        return {"dp": ((x * 4 + y) * 4 + z) * 2 + c}

    def step(self, dim, by):
        return self.dev(**{dim: lax.rem(getattr(self, dim) + by, 4)})

    def group(self):
        out = []
        for dz in (2, 1, 3):
            zz = lax.rem(self.z + dz, 4)
            out += [(zz, self.c), (zz, 1 - self.c)]
        return [*out, (self.z, 1 - self.c)]

    def barrier(self):
        sem = pltpu.get_barrier_semaphore()
        peers = [self.dev(z=z, c=c) for z, c in self.group()]
        peers += [self.step(d, by) for d in ("x", "y") for by in (1, 3)]
        for peer in peers:
            pl.semaphore_signal(sem, inc=1, device_id=peer, device_id_type=pl.DeviceIdType.MESH)
        pl.semaphore_wait(sem, len(peers))


class Sender:
    def __init__(self, send, recv):
        self.send, self.recv, self.n, self.groups, self.shared = send, recv, 0, {}, {}

    def start(self, src, dst, device, group, together=None):
        mine = self.groups.setdefault(group, len(self.groups))
        if together is None or together not in self.shared:
            got = self.n
            self.n += 1
            if together is not None:
                self.shared[together] = got
        else:
            got = self.shared[together]
        copy = pltpu.make_async_remote_copy(
            src_ref=src,
            dst_ref=dst,
            send_sem=self.send.at[mine],
            recv_sem=self.recv.at[got],
            device_id=device,
            device_id_type=pl.DeviceIdType.MESH,
        )
        copy.start()
        return copy

    def arrived(self, together, like):
        pltpu.make_async_copy(like, like, self.recv.at[self.shared[together]]).wait()

    def drain(self, sizes):
        for group, n in self.groups.items():
            like = sizes[group]
            pltpu.make_async_copy(like, like, self.send.at[n]).wait()


def rows(start, n):
    return pl.ds(pl.multiple_of(start, GROUP), n)


def total(refs, sl):
    acc = refs[0][sl].astype(F32)
    for r in refs[1:]:
        acc = acc + r[sl].astype(F32)
    return acc


def vadd(dst, refs, n, step):
    def body(i, carry):
        sl = (rows(i * step, step), ALL)
        dst[sl] = total(refs, sl).astype(dst.dtype)
        return carry

    lax.fori_loop(0, n // step, body, 0)


def interleave(plan, release, **programs):
    live = dict(programs)

    def advance(n):
        try:
            next(live[n])
        except StopIteration:
            del live[n]

    for n in plan:
        if n in release:
            release[n]()
        elif n in live:
            advance(n)
    while live:
        for n in list(live):
            advance(n)


def step_kernel(g_gate, g_up, g_down, w_gate, w_up, w_down, m_gate, m_up, m_down, v_gate, v_up, v_down,
                o_a, o_b, o_c, om_gate, om_up, om_down, ov_gate, ov_up, ov_down,
                own_a, own_b, own_c, ra, rb, rc, s1a, s2a, s1b, s2b, s1c, s2c, tc, f_a, f_b, f_c,
                snd_a, snd_b, snd_c, rcv_a, rcv_b, rcv_c, new_a, new_b, new_c, got_a, got_b, got_c,
                wb_gate, wb_up, wb_down, fw_wide, fw_tall, pk_a, pk_b, pk_c, sw_a, sw_b, sw_c, sm_a, sm_b, sm_c, sv_a, sv_b, sv_c, w2_gate, w2_up, w2_down, m2_gate, m2_up, m2_down, v2_gate, v2_up, v2_down,
                send, recv, local):
    at = Place()
    x, y, z, c = at.x, at.y, at.z, at.c
    net = Sender(send, recv)
    loads = [0]
    rel = lambda base, j: lax.rem(base + OFF[j], 4)
    cols = lambda start, n: pl.ds(pl.multiple_of(start, LANES), n)

    def item_a(ref, k, j):
        return ref.at[rows(SLAB * k + BLOCK * rel(y, j), BLOCK), :]

    def item_b(ref, k, j):
        return ref.at[rows(TALL * k + TALL4 * rel(x, j), TALL), :]

    def item_c(ref, k, j):
        return ref.at[k, rows(SLAB * rel(x, j), SLAB), :]

    def moves_a(layer, ref, k, j):
        sl = rows(SLAB * k + BLOCK * rel(y, j), BLOCK)
        return [(g_up.at[0, layer, sl, pl.ds(0, UA)], ref.at[sl, pl.ds(0, UA)])]

    def moves_b(layer, ref, k, j):
        return [(g_down.at[0, layer, rows(TALL * k + TALL4 * rel(x, j), TALL), :], item_b(ref, k, j))]

    def moves_c(layer, ref, k, j):
        sl = rows(SLAB * rel(x, j), SLAB)
        out = [(g_gate.at[0, layer, sl, cols(WIN * k, WIN)], ref.at[k, sl, pl.ds(0, WIN)])]
        if UC:
            out.append((g_up.at[0, layer, sl, cols(UA + UC * k, UC)], ref.at[k, sl, pl.ds(WIN, UC)]))
        return out

    par_a, par_b, par_c = o_a.at[1 - c], o_b.at[1 - c], o_c.at[1 - c]
    there = {"a": o_a.at[c], "b": o_b.at[c], "c": o_c.at[c]}
    colours = {
        "c": (own_c, par_c, item_c, moves_c, z, "z", rc, SLAB, 32),
        "a": (own_a, par_a, item_a, moves_a, x, "x", ra, BLOCK, GROUP),
        "b": (own_b, par_b, item_b, moves_b, y, "y", rb, TALL, BLOCK),
    }

    locals_ = {}

    def load(src, dst, together):
        n = locals_.setdefault(together, len(locals_))
        pltpu.make_async_copy(src, dst, local.at[n]).start()

    def loaded(together, like):
        pltpu.make_async_copy(like, like, local.at[locals_[together]]).wait()

    sets = (((2, 0),), ((2, 2),), ((1, 2), (3, 0)), ((1, 0), (3, 2)), ((2, 1), (2, 3)), ((1, 3), (3, 1)), ((0, 0), (0, 2)), ((1, 1), (3, 3), (0, 1), (0, 3)))
    tail = (ALL, pl.ds(EDGE, LANES)), (ALL, pl.ds(UA, LANES))
    wide, tall = rows(SLAB * x + BLOCK * y, BLOCK), rows(TALL4 * x + TALL * y, TALL)
    state = [(w_gate.at[:, wide, :], wb_gate), (w_up.at[:, wide, :], wb_up), (w_down.at[:, tall, :], wb_down)]
    moments = ((m_gate, om_gate, m2_gate), (m_up, om_up, m2_up), (m_down, om_down, m2_down),
               (v_gate, ov_gate, v2_gate), (v_up, ov_up, v2_up), (v_down, ov_down, v2_down))
    state += [(src, dst) for src, dst, _ in moments]
    load(g_gate.at[(0, c, *tail[0])], own_a.at[tail[1]], "tail")
    for i, part in enumerate(sets):
        for dk, j in part:
            for n, (own, par, item, moves, k0, *_) in colours.items():
                for src, dst in moves(c, own, lax.rem(k0 + dk, 4), j):
                    load(src, dst, (n, i))
    for i, (src, dst) in enumerate(state):
        load(src, dst, ("state", i))
    at.barrier()
    net.start(g_gate.at[(0, 1 - c, *tail[0])], there["a"].at[tail[1]], at.partner, "da", "tail")
    for i, part in enumerate(sets):
        for dk, j in part:
            for n, (own, par, item, moves, k0, *_) in colours.items():
                for src, dst in moves(1 - c, there[n], lax.rem(k0 + dk, 4), j):
                    net.start(src, dst, at.partner, "d" + n, (n, i))
    here_is = set()

    def here_now(n, dk, j):
        i = [i for i, part in enumerate(sets) if (dk, j) in part][0]
        if (n, i) in here_is:
            return
        here_is.add((n, i))
        count = len(sets[i])
        if n == "a":
            like = own_a.at[pl.ds(0, BLOCK * count), pl.ds(0, UA)]
        elif n == "b":
            like = own_b.at[pl.ds(0, TALL * count), :]
        else:
            like = own_c.at[0, pl.ds(0, SLAB * count), :]
        loaded((n, i), like)
        net.arrived((n, i), like)

    def first(n):
        own, par, item, moves, k0, dim, r, height, step = colours[n]
        up, down = at.step(dim, 1), at.step(dim, 3)
        k2, kp, km = (lax.rem(k0 + d, 4) for d in (2, 1, 3))
        one = {}
        if n == "a":
            like = own_a.at[:, pl.ds(0, LANES)]
            loaded("tail", like)
            net.arrived("tail", like)

        def opposite(j):
            here_now(n, 2, j)
            here = item(own, k2, j)
            vadd(here, (here, item(par, k2, j)), height, step)
            one[j] = net.start(here, r.at[j], up if j < 2 else down, "f" + n)

        def beside(dk, j, more):
            here_now(n, dk, j)
            if more:
                one[j].wait_recv()
            here = item(own, kp if dk == 1 else km, j)
            par_here = item(par, kp if dk == 1 else km, j)
            vadd(here, (here, par_here, r.at[j]) if more else (here, par_here), height, step)
            net.start(here, r.at[4 + j if dk == 1 else GROUP + j], up if dk == 1 else down, "f" + n, (n, "two", j))

        def mine(j):
            here_now(n, 0, j)
            net.arrived((n, "two", j), r.at[pl.ds(0, 2)])
            here = item(own, k0, j)
            vadd(here, (here, item(par, k0, j), r.at[4 + j], r.at[GROUP + j]), height, step)

        opposite(0)
        yield
        opposite(2)
        yield
        beside(1, 2, False)
        yield
        beside(3, 0, False)
        yield
        beside(1, 0, True)
        yield
        beside(3, 2, True)
        yield
        opposite(1)
        yield
        opposite(3)
        yield
        beside(1, 3, False)
        yield
        beside(3, 1, False)
        yield
        mine(0)
        yield 0
        mine(2)
        yield 2
        beside(1, 1, True)
        yield
        beside(3, 3, True)
        yield
        mine(1)
        yield 1
        mine(3)
        yield 3

    def later(n, dim, block, halves, r1, r2, ready, hold, step, done):
        up, down = at.step(dim, 1), at.step(dim, 3)
        waiting = []
        for i, chunk in enumerate(ready):
            if chunk is not None:
                waiting.append(chunk)
            while waiting and i >= hold:
                j = waiting.pop(0)
                if j == 0:
                    a = net.start(halves(block(0), 0), halves(r1.at[0], 0, True), up, n)
                    b = net.start(halves(block(0), 1), halves(r1.at[1], 1, True), down, n)
                if j == 2:
                    net.start(halves(block(2), 1), halves(r2.at[0], 1), up, n, n)
                if j == 1:
                    net.start(halves(block(1), 0), halves(r2.at[1], 0), down, n, n)
            yield
        a.wait_recv()
        here = halves(block(2), 0)
        vadd(here, (here, halves(r1.at[0], 0, True)), here.shape[0], GROUP)
        net.start(here, halves(r2.at[0], 0), up, n, n)
        yield
        b.wait_recv()
        here = halves(block(1), 1)
        vadd(here, (here, halves(r1.at[1], 1, True)), here.shape[0], GROUP)
        net.start(here, halves(r2.at[1], 1), down, n, n)
        yield
        net.arrived(n, r2)
        vadd(done, (block(3), r2.at[0], r2.at[1]), block(3).shape[0], step)

    def by_cols(w):
        def cut(ref, h, packed=False):
            return ref if packed else ref.at[:, pl.ds(h * w, w)]

        return cut

    def by_rows(n0, n1):
        def cut(ref, h, packed=False):
            return ref.at[pl.ds(0, (n0, n1)[h]), :] if packed else ref.at[pl.ds((0, n0)[h], (n0, n1)[h]), :]

        return cut

    def spread(n, full, blocks, packed, snd, rcv):
        for k in range(GROUP):
            for t in range(full.shape[1] // LANES):
                packed[k, pl.ds(blocks * t, blocks), :] = full[pl.ds(blocks * k, blocks), pl.ds(LANES * t, LANES)]
            snd[k] = packed[k].astype(BF)
        for zz, cc in at.group():
            s = 2 * zz + cc
            net.start(snd.at[s], rcv.at[at.g], at.dev(z=zz, c=cc), "s" + n, "s" + n)
        rcv[at.g] = snd[at.g]

    def prepare():
        for ref in (sw_a, sw_b, sw_c, sm_a, sm_b, sm_c, sv_a, sv_b, sv_c):
            ref[...] = jnp.zeros(ref.shape, F32)
        for i, (_, dst) in enumerate(state):
            loaded(("state", i), dst)
        yield
        fw_wide[pl.ds(BLOCK, GROUP), :] = jnp.zeros((GROUP, FF), F32)
        fw_tall[pl.ds(TALL, GROUP), :] = jnp.zeros((GROUP, D), F32)
        for block, full, out, n, height in ((wb_gate, fw_wide, w2_gate, OWN_A, GROUP), (wb_up, fw_wide, w2_up, OWN_A, GROUP), (wb_down, fw_tall, w2_down, OWN_B, 32)):
            for layer in range(2):
                full[pl.ds(0, GROUP * n), :] = block[layer].astype(F32)
                for k in range(GROUP):

                    @pl.when(at.g == k)
                    def _():
                        out[layer] = full[pl.ds(n * k, height), :]

                yield
        for _, src, out in moments:
            for r in range(src.shape[0]):
                for layer in range(2):
                    out[layer, pl.ds(r, 1), :] = src[r, pl.ds(layer, 1), :]
            yield
        for which in kept:
            for to, here, there in tiles(*which):
                here[to] = there[...]
            yield

    def tiles(wide_gate, wide_up, tall, in_a, in_b, in_c):
        for layer in range(2):
            for t in range(OWN_B):
                piece = (layer, pl.ds(0, OWN_A), pl.ds(LANES * t, LANES))
                if t < 24:
                    yield (layer, t // 6, pl.ds(OWN_A * (t % 6), OWN_A)), in_c, wide_gate.at[piece]
                else:
                    yield (layer, pl.ds(OWN_A * (UA // LANES), OWN_A)), in_a, wide_gate.at[piece]
                if t < UA // LANES:
                    yield (layer, pl.ds(OWN_A * t, OWN_A)), in_a, wide_up.at[piece]
                else:
                    yield (layer, (t - UA // LANES) // SHARE, pl.ds(OWN_A * (6 + (t - UA // LANES) % SHARE), OWN_A)), in_c, wide_up.at[piece]
            for t in range(OWN_A):
                yield (layer, pl.ds(OWN_B * t, OWN_B)), in_b, tall.at[layer, pl.ds(0, OWN_B), pl.ds(LANES * t, LANES)]

    kept = (
        (w2_gate, w2_up, w2_down, sw_a, sw_b, sw_c),
        (m2_gate, m2_up, m2_down, sm_a, sm_b, sm_c),
        (v2_gate, v2_up, v2_down, sv_a, sv_b, sv_c),
    )
    updated = []

    def finish():
        assert len(updated) == 3
        for which in kept[1:]:
            for to, here, there in tiles(*which):
                there[...] = here[to]
            yield
        for _, out, src in moments:
            for r in range(out.shape[0]):
                for layer in range(2):
                    out[r, pl.ds(layer, 1), :] = src[layer, pl.ds(r, 1), :]
            yield

    def update(state, at_, g, new):
        w2, m2, v2 = state
        new[at_], m2[at_], v2[at_] = adamw(w2[at_], m2[at_], v2[at_], g)

    def summed(rcv, layer):
        acc = rcv[layer].astype(F32)
        for zz in range(1, 4):
            acc = acc + rcv[2 * zz + layer].astype(F32)
        return acc.astype(BF).astype(F32)

    def step_a():
        for layer in range(2):
            update((sw_a, sm_a, sv_a), layer, summed(rcv_a, layer), new_a)

    def step_b():
        for layer in range(2):
            update((sw_b, sm_b, sv_b), layer, summed(rcv_b, layer), new_b)

    def step_c():
        for layer in range(2):
            for zz in range(4):
                update((sw_c, sm_c, sv_c), (layer, zz), rcv_c[2 * zz + layer].astype(F32), new_c)

    def over(n, ref):
        net.start(ref, ref, at.partner, "x" + n, "x" + n)

    def share(n, new, got):
        for zz, cc in at.group():
            one = new.at[cc, zz] if n == "c" else new.at[cc]
            net.start(one, got.at[at.g], at.dev(z=zz, c=cc), "w" + n, "w" + n)
        got[at.g] = new[c, z] if n == "c" else new[c]

    def build(n, blocks, got, full, out):
        net.arrived("w" + n, got.at[pl.ds(0, OTHERS)])
        for k in range(GROUP):
            one = got[k].astype(F32)
            for t in range(full.shape[1] // LANES):
                full[pl.ds(blocks * k, blocks), pl.ds(LANES * t, LANES)] = one[blocks * t : blocks * (t + 1)]
        out[...] = full[pl.ds(0, GROUP * blocks), :].astype(BF)

    release = {}

    def small(n, dim, block, halves):
        up, down = at.step(dim, 1), at.step(dim, 3)
        mine = block(3)
        m0 = net.start(halves(mine, 0), halves(mine, 0), up, n)
        p1 = net.start(halves(mine, 1), halves(mine, 1), down, n)
        m1 = net.start(halves(mine, 1), halves(mine, 1), up, n)
        p0 = net.start(halves(mine, 0), halves(mine, 0), down, n)
        yield 3
        m0.wait_recv()
        here = halves(block(1), 0)
        net.start(here, here, up, n, n)
        p1.wait_recv()
        here = halves(block(2), 1)
        net.start(here, here, down, n, n)
        yield
        m1.wait_recv()
        yield 1
        p0.wait_recv()
        yield 2
        net.arrived(n, mine)
        yield 0

    def large(n, dim, k0, item, ready):
        up, down = at.step(dim, 1), at.step(dim, 3)
        kp, km, k2 = (lax.rem(k0 + d, 4) for d in (1, 3, 2))
        fm, fp, order, held = {}, {}, [], []

        def flush():
            if held:
                j = held.pop(0)
                here = item(k0, j)
                fm[j] = net.start(here, here, up, "l" + n)
                fp[j] = net.start(here, here, down, "l" + n)
                over(n, here)
                order.append(j)

        release[n.upper()] = flush
        for j in ready:
            if j is not None:
                held.append(j)
            yield
        while held:
            flush()
            yield
        f2 = {}
        for j in order:
            fm[j].wait_recv()
            here = item(km, j)
            if j < 2:
                f2[j] = net.start(here, here, up, "l" + n)
            over(n, here)
            yield
            fp[j].wait_recv()
            here = item(kp, j)
            if j >= 2:
                f2[j] = net.start(here, here, down, "l" + n)
            over(n, here)
            yield
        for j in order:
            f2[j].wait_recv()
            over(n, item(k2, j))
            yield

    def colour_a():
        pk_a[...] = jnp.zeros(pk_a.shape, F32)
        yield from later("ma", "y", lambda j: item_a(own_a, x, j), by_cols(WA // 2), s1a, s2a, first("a"), 0, GROUP, f_a)
        spread("a", f_a, OWN_A, pk_a, snd_a, rcv_a)
        yield
        net.arrived("sa", rcv_a.at[pl.ds(0, OTHERS)])
        step_a()
        updated.append("a")
        share("a", new_a, got_a)
        yield
        out = lambda k, j: item_a(o_a.at[c], k, j)
        build("a", OWN_A, got_a, f_a, out(x, 3))
        yield from large("a", "x", x, out, small("ga", "y", lambda j: out(x, j), by_cols(WA // 2)))

    def colour_b():
        pk_b[...] = jnp.zeros(pk_b.shape, F32)
        yield from later("mb", "x", lambda j: item_b(own_b, y, j), by_rows(104, 96), s1b, s2b, first("b"), 13, BLOCK, f_b)
        spread("b", f_b, OWN_B, pk_b, snd_b, rcv_b)
        yield
        net.arrived("sb", rcv_b.at[pl.ds(0, OTHERS)])
        step_b()
        updated.append("b")
        share("b", new_b, got_b)
        yield
        out = lambda k, j: item_b(o_b.at[c], k, j)
        build("b", OWN_B, got_b, f_b, out(y, 3))
        yield from large("b", "y", y, out, small("gb", "x", lambda j: out(y, j), by_rows(104, 96)))

    def colour_c():
        pk_c[...] = jnp.zeros(pk_c.shape, F32)
        yield from later("mc", "x", lambda j: item_c(own_c, z, j), by_rows(80, 80), s1c, s2c, first("c"), 13, 32, item_c(own_c, z, 3))
        part = lambda ref, yy: ref.at[z, rows(SLAB * x + BLOCK * yy, BLOCK), :]
        for d in (2, 1, 3):
            yy = lax.rem(y + d, 4)
            net.start(part(own_c, yy), tc.at[d - 1], at.step("y", d), "nc", "nc")
        yield
        net.arrived("nc", tc)
        vadd(f_c, (part(own_c, y), *(tc.at[d] for d in range(3))), BLOCK, GROUP)
        spread("c", f_c, OWN_A, pk_c, snd_c, rcv_c)
        yield
        net.arrived("sc", rcv_c.at[pl.ds(0, OTHERS)])
        step_c()
        updated.append("c")
        share("c", new_c, got_c)
        yield
        out = lambda k, j: item_c(o_c.at[c], k, j)
        mine = part(o_c.at[c], y)
        build("c", OWN_A, got_c, f_c, mine)
        for d in (2, 1, 3):
            net.start(mine, mine, at.step("y", d), "hc", "hc")
        yield
        net.arrived("hc", tc)
        yield from large("c", "z", z, out, small("gc", "x", lambda j: out(z, j), by_rows(80, 80)))

    interleave(PLAN, release, c=colour_c(), a=colour_a(), b=colour_b(), p=prepare(), f=finish())
    for n, (own, *_) in colours.items():
        net.arrived("x" + n, own)
    sizes = {"nc": tc, "hc": tc}
    for n, (own, _, _, _, _, _, r, *_) in colours.items():
        sizes |= {"d" + n: own, "x" + n: own, "f" + n: r, "l" + n: r, "m" + n: r.at[pl.ds(0, 3)], "g" + n: r.at[pl.ds(0, 3)]}
    for n, rcv in (("a", rcv_a), ("b", rcv_b), ("c", rcv_c)):
        sizes |= {"s" + n: rcv.at[pl.ds(0, OTHERS)], "w" + n: rcv.at[pl.ds(0, OTHERS)]}
    net.drain(sizes)
    assert (net.n, len(net.groups), len(locals_)) == (RECV, SEND, LOCAL), (net.n, len(net.groups), len(locals_))


def write_kernel(a, b, c, *refs):
    small, (gate, up, down), outs, sem = refs[:6], refs[6:9], refs[9:15], refs[15]
    copies = [(b.at[l], down.at[l]) for l in range(2)]
    copies += [(a.at[l, :, pl.ds(0, UA)], up.at[l, :, pl.ds(0, UA)]) for l in range(2)]
    copies += [(c.at[l, k, :, pl.ds(0, WIN)], gate.at[l, :, pl.ds(WIN * k, WIN)]) for l in range(2) for k in range(4)]
    copies += [(a.at[l, :, pl.ds(UA, LANES)], gate.at[l, :, pl.ds(EDGE, LANES)]) for l in range(2)]
    if UC:
        copies += [(c.at[l, k, :, pl.ds(WIN, UC)], up.at[l, :, pl.ds(UA + UC * k, UC)]) for l in range(2) for k in range(4)]
    copies += list(zip(small, outs, strict=True))
    for src, dst in copies:
        pltpu.make_async_copy(src, dst, sem).start()
    for out in (gate, up, down, *outs):
        pltpu.make_async_copy(out, out, sem).wait()


def spec(space, n):
    return [pl.BlockSpec(memory_space=space)] * n


def solution(mesh):
    def step(*arrays):
        terms, weights, m, v = (arrays[i : i + 3] for i in (0, 3, 6, 9))
        turn = lambda one: jnp.transpose(one, (1, 0, 2))
        moments = [turn(one) for one in (*m, *v)]
        own_rows = [(2, GROUP, FF), (2, GROUP, FF), (2, 32, D)]
        blocks = [(GROUP, PACK_A, LANES), (GROUP, PACK_B, LANES), (GROUP, PACK_C, LANES)]
        states = [(2, PACK_A, LANES), (2, PACK_B, LANES), (2, 4, PACK_C, LANES)]
        results = pl.pallas_call(
            step_kernel,
            out_shape=[
                VMEM((2, D, WA), BF),
                VMEM((2, FF, D), BF),
                VMEM((2, 4, D, WC), BF),
                *[VMEM(one.shape, F32) for one in moments],
            ],
            in_specs=spec(HBM, 12),
            out_specs=spec(VMEM, 9),
            scratch_shapes=[
                VMEM((D, WA), BF),
                VMEM((FF, D), BF),
                VMEM((4, D, WC), BF),
                *[VMEM((12, *s), BF) for s in ((BLOCK, WA), (TALL, D), (SLAB, WC))],
                VMEM((2, BLOCK, WA // 2), BF),
                VMEM((2, BLOCK, WA), BF),
                VMEM((2, 104, D), BF),
                VMEM((2, TALL, D), BF),
                VMEM((2, 80, WC), BF),
                VMEM((2, SLAB, WC), BF),
                VMEM((3, BLOCK, WC), BF),
                VMEM((BLOCK_PAD, WA), F32),
                VMEM((TALL_PAD, D), F32),
                VMEM((BLOCK_PAD, WC), F32),
                *[VMEM(s, BF) for s in blocks] * 2,
                *[VMEM(s, BF) for s in states],
                *[VMEM(s, BF) for s in blocks],
                VMEM((2, BLOCK, FF), BF),
                VMEM((2, BLOCK, FF), BF),
                VMEM((2, TALL, D), BF),
                VMEM((BLOCK_PAD, FF), F32),
                VMEM((TALL_PAD, D), F32),
                *[VMEM(s, F32) for s in blocks],
                *[VMEM(s, F32) for s in states] * 3,
                *[VMEM(s, F32) for s in own_rows] * 3,
                pltpu.SemaphoreType.DMA((SEND,)),
                pltpu.SemaphoreType.DMA((RECV,)),
                pltpu.SemaphoreType.DMA((LOCAL,)),
            ],
            compiler_params=pltpu.CompilerParams(collective_id=0, has_side_effects=True, vmem_limit_bytes=36 * 2**20),
            name="step",
        )(*terms, *weights, *moments)
        done = pl.pallas_call(
            write_kernel,
            out_shape=[jax.ShapeDtypeStruct(w.shape, BF) for w in weights] + [jax.ShapeDtypeStruct(one.shape, F32) for one in moments],
            in_specs=spec(VMEM, 9),
            out_specs=spec(HBM, 9),
            scratch_shapes=[pltpu.SemaphoreType.DMA],
            compiler_params=pltpu.CompilerParams(vmem_limit_bytes=2**20),
            name="write",
        )(*results)
        return (*done[:3], *(turn(one) for one in done[3:]))

    all_of, cut = P(None, None, None), P(None, "dp", None)
    return jax.shard_map(
        step,
        mesh=mesh,
        in_specs=(P(("rep", "dp"), None, None, None),) * 3 + (all_of,) * 3 + (cut,) * 6,
        out_specs=(P("rep", None, None),) * 3 + (P("rep", "dp", None),) * 6,
        check_vma=False,
    )
```
